32 devices in a mesh: rep: 4 (over x, y), dp: 8 (over z, core).
Axes of the slice: x: 2, y: 2, z: 4, core: 2. Of those that a mesh axis runs over, the one named last changes fastest.
Arguments:
- g_w_gate: bfloat16 [32, 2, 1152, 4608], P(('rep', 'dp')), parts along dimension 0
- g_w_up: bfloat16 [32, 2, 1152, 4608], P(('rep', 'dp')), parts along dimension 0
- g_w_down: bfloat16 [32, 2, 4608, 1152], P(('rep', 'dp')), parts along dimension 0
- w_gate: bfloat16 [2, 1152, 4608], replicated
- w_up: bfloat16 [2, 1152, 4608], replicated
- w_down: bfloat16 [2, 4608, 1152], replicated
- m_w_gate: float32 [2, 1152, 4608], P(None, 'dp')
- m_w_up: float32 [2, 1152, 4608], P(None, 'dp')
- m_w_down: float32 [2, 4608, 1152], P(None, 'dp')
- v_w_gate: float32 [2, 1152, 4608], P(None, 'dp')
- v_w_up: float32 [2, 1152, 4608], P(None, 'dp')
- v_w_down: float32 [2, 4608, 1152], P(None, 'dp')
Outputs:
- output 1: bfloat16 [8, 1152, 4608], P('rep'), parts along dimension 0
- output 2: bfloat16 [8, 1152, 4608], P('rep'), parts along dimension 0
- output 3: bfloat16 [8, 4608, 1152], P('rep'), parts along dimension 0
- output 4: float32 [8, 1152, 4608], P('rep', 'dp'), parts along dimension 0
- output 5: float32 [8, 1152, 4608], P('rep', 'dp'), parts along dimension 0
- output 6: float32 [8, 4608, 1152], P('rep', 'dp'), parts along dimension 0
- output 7: float32 [8, 1152, 4608], P('rep', 'dp'), parts along dimension 0
- output 8: float32 [8, 1152, 4608], P('rep', 'dp'), parts along dimension 0
- output 9: float32 [8, 4608, 1152], P('rep', 'dp'), parts along dimension 0
There are 4 independent parts. The reference program is written for one: setup_inputs(seed, part) draws one part's arguments, and reference() takes and returns one part's arrays. A program takes and returns all parts, laid end to end along the dimension named above; an argument that names none is the same for every part.
All inputs are finite; a program needn't handle non-finite values.
Results may differ from the reference program's by a relative error of at most 0.022.
Values are sent between devices in bfloat16 or wider.
A program may use at most 2 GiB of HBM per device.

```python
import jax
import jax.numpy as jnp
from jax import lax

DEVICES = 8
D = 1152
FF = 4608
LAYERS = 2
NAMES = ("w_gate", "w_up", "w_down")
SHAPES = {"w_gate": (LAYERS, D, FF), "w_up": (LAYERS, D, FF), "w_down": (LAYERS, FF, D)}


def setup_inputs(seed: int = 0, part: int = 0) -> dict:
    kz, *keys = jax.random.split(jax.random.key(seed), 1 + 5 * len(NAMES))
    loud = 2.0 ** jax.random.uniform(kz, (), jnp.float32, -1.0, 1.0)
    drawn = {}
    for name, key, both in zip(NAMES, keys[:3], keys[3:6], strict=True):
        own = jax.random.normal(jax.random.fold_in(key, part), (DEVICES, *SHAPES[name]), jnp.float32)
        shared = jax.random.normal(jax.random.fold_in(both, part), SHAPES[name], jnp.float32)
        drawn["g_" + name] = (loud * (0.7 * shared / DEVICES + 0.7 * own * DEVICES**-0.5)).astype(jnp.bfloat16)
    for name, key in zip(NAMES, keys[6:9], strict=True):
        drawn[name] = (jax.random.normal(key, SHAPES[name], jnp.float32) * SHAPES[name][1] ** -0.5).astype(jnp.bfloat16)
    for name, key in zip(NAMES, keys[9:12], strict=True):
        drawn["m_" + name] = loud * 0.5 * jax.random.normal(key, SHAPES[name], jnp.float32)
    for name, key in zip(NAMES, keys[12:15], strict=True):
        drawn["v_" + name] = loud * loud * jax.random.uniform(key, SHAPES[name], jnp.float32, 0.5, 1.5)
    return drawn


def adamw(w, m, v, g):
    m = 0.9 * m + 0.1 * g
    v = 0.95 * v + 0.05 * g * g
    step = m * lax.rsqrt(v + 1e-8) + 0.1 * w
    return (w - 0.02 * step).astype(jnp.bfloat16), m, v


def reference(g_w_gate, g_w_up, g_w_down, w_gate, w_up, w_down, m_w_gate, m_w_up, m_w_down, v_w_gate, v_w_up, v_w_down):
    def total(terms):
        return lax.scan(lambda so_far, term: (so_far + term.astype(jnp.float32), None), jnp.zeros(terms.shape[1:], jnp.float32), terms)[0]

    gradients = [total(terms).astype(jnp.bfloat16).astype(jnp.float32) for terms in (g_w_gate, g_w_up, g_w_down)]
    new = [
        adamw(w.astype(jnp.float32), m, v, g)
        for w, m, v, g in zip((w_gate, w_up, w_down), (m_w_gate, m_w_up, m_w_down), (v_w_gate, v_w_up, v_w_down), gradients, strict=True)
    ]
    return tuple(one[which] for which in range(3) for one in new)
```

```python
import functools

import jax
import jax.numpy as jnp
from jax import lax
from jax.experimental import pallas as pl
from jax.experimental.pallas import tpu as pltpu
from jax.sharding import PartitionSpec as P

MESH = pl.DeviceIdType.MESH
ROWS = 16
LAYERS = 2
CHIPS = 4
K = 4
KA = 4
LAG = 2
END = 3
D = 2
PF = 3
RING = 4
FR = 3
MOVE = 8
PRE = 4
PS = 8
PG = 3
G = 6
SLOTS = 24


def adamw(w, m, v, g):
    m = 0.9 * m + 0.1 * g
    v = 0.95 * v + 0.05 * g * g
    step = m * lax.rsqrt(v + 1e-8) + 0.1 * w
    return (w - 0.02 * step).astype(jnp.bfloat16), m, v


def kernel(geo, *refs):
    C, CD, NR, NC, CB = geo
    R = C // CD
    E = 4 * NC
    g, w, m, v = refs[0:3], refs[3:6], refs[6:9], refs[9:12]
    W, M, V, PT = refs[12:15], refs[15:18], refs[18:21], refs[21:24]
    (land, own, par, out, mb, vb, wb, wn, recv, credits, send, gsend, ownsem, parsem, d2d_recv, d2d_send, ld_sem, ww_sem,
     ag_recv, ag_send) = refs[24:]
    rep = lax.axis_index("rep")
    me = lax.axis_index("dp")
    z, c = me // 2, me % 2
    partner = (rep, z * 2 + 1 - c)
    nexts = ((rep, jnp.minimum(z + 1, CHIPS - 1) * 2 + c), (rep, jnp.maximum(z - 1, 0) * 2 + c))
    qs = (z, CHIPS - 1 - z)

    def split(j):
        mat = j // NR
        return mat // LAYERS, mat % LAYERS, j % NR

    def by_weight(j, body):
        k, l, r = split(j)
        for i in range(3):
            @pl.when(k == i)
            def _(i=i):
                body(i, l, r)

    def rows(i, dev, r):
        n = ROWS if i < 2 else ROWS * R
        return pl.ds(pl.multiple_of((dev * NR + r) * n, n), n)

    def load(i, src, dst, sem):
        if i < 2:
            pltpu.make_async_copy(src, dst, sem).start()
        else:
            for s in range(R):
                pltpu.make_async_copy(src.at[pl.ds(s * ROWS, ROWS), :], dst.at[:, pl.ds(s * CD, CD)], sem).start()

    def save(i, src, dst, sem):
        if i < 2:
            pltpu.make_async_copy(src, dst, sem).start()
        else:
            for s in range(R):
                pltpu.make_async_copy(src.at[:, pl.ds(s * CD, CD)], dst.at[pl.ds(s * ROWS, ROWS), :], sem).start()

    def wait_local(buf, sem):
        pltpu.make_async_copy(buf, buf, sem).wait()

    def decode(e):
        p = e - NC
        x = p - D
        first, last, head, tail = p < 0, p >= 2 * NC, p < D, p >= 2 * NC - D
        beta = jnp.where(first, 3, jnp.where(last, 0, jnp.where(head, 2, jnp.where(tail, 1, 1 + x % 2))))
        mid = jnp.where(x % 2 == 0, x // 2, D + x // 2)
        j = jnp.where(first, e, jnp.where(last, p - 2 * NC, jnp.where(head, p, jnp.where(tail, p - NC, mid))))
        return beta, j

    def sums(e, q):
        beta, j = decode(e)
        return (e >= 0) & (e < E) & ((q < beta) | ((q == beta) & (beta % 2 == 1))), beta, j

    def pair_index(b, i):
        n = NC // PG
        return jnp.where((b == 0) | (b == 3), 2 * i + jnp.where(b == 0, 1, 0), 2 * n + 2 * i + jnp.where(b == 1, 1, 0))

    def pair_group(i):
        n = NC // PG
        late = i >= 2 * n
        odd = i % 2
        b = jnp.where(late, 2 - odd, 3 - 3 * odd)
        return b, jnp.where(late, i - 2 * n, i) // 2

    def pair_wait(sem):
        many = land.at[0, pl.ds(0, PG)]
        pltpu.make_async_copy(many, many, sem).wait()

    def pair_push(i):
        @pl.when(i < 4 * NC // PG)
        def _():
            @pl.when(i >= PS)
            def _():
                pair_wait(d2d_send.at[i % PS])
            b, group = pair_group(i)

            def go(k, l, r):
                n = (ROWS if k < 2 else ROWS * R) * PG
                src = pl.ds(pl.multiple_of(((2 * b + 1 - c) * NR + r) * (n // PG), n), n)
                dst = pl.ds(pl.multiple_of(r * (n // PG), n), n)
                pltpu.make_async_remote_copy(
                    g[k].at[0, l, src, :], PT[k].at[l, b, dst, :], d2d_send.at[i % PS], d2d_recv.at[i],
                    device_id=partner, device_id_type=MESH).start()

            by_weight(group * PG, go)

    def prefetch(d, e):
        need, beta, j = sums(e, qs[d])
        b = beta if d == 0 else CHIPS - 1 - beta

        @pl.when(need)
        def _():
            s = e % RING
            by_weight(j, lambda k, l, r: load(k, g[k].at[0, l, rows(k, 2 * b + c, r), :], own.at[d, s], ownsem.at[d, s]))

            @pl.when(j % PG == 0)
            def _():
                pair_wait(d2d_recv.at[pair_index(b, j // PG)])

            by_weight(j, lambda k, l, r: load(k, PT[k].at[l, b, rows(k, 0, r), :], par.at[d, s], parsem.at[d, s]))

    def step_load(j):
        @pl.when(j < NC)
        def _():
            s = j % FR

            def go(k, l, r):
                load(k, m[k].at[l, rows(k, 0, r), :], mb.at[s], ld_sem.at[0, s])
                load(k, v[k].at[l, rows(k, 0, r), :], vb.at[s], ld_sem.at[1, s])
                load(k, w[k].at[l, rows(k, me, r), :], wb.at[s], ld_sem.at[2, s])

            by_weight(j, go)

    def wait_sum(d, n):
        pltpu.make_async_copy(out.at[d, 0], out.at[d, 0], send.at[d, n % K]).wait()

    def wait_gather(d, n):
        pltpu.make_async_copy(out.at[d, 0], out.at[d, 0], gsend.at[d, n % KA]).wait()

    def wait_recv(d, n):
        pltpu.make_async_copy(land.at[d, 0], land.at[d, 0], recv.at[d, n % SLOTS]).wait()

    def credit(d, n):
        @pl.when((n >= SLOTS) & (n % G == 0))
        def _():
            pl.semaphore_wait(credits.at[d], 1)

    def columns(body):
        def step(i, _):
            body(pl.ds(pl.multiple_of(i * CB, CB), CB))
            return 0

        lax.fori_loop(0, C // CB, step, 0)

    def weight(k, l, dev, r):
        return W[k].at[l, rows(k, dev, r), :]

    def gather_send(d, j, dev, i, n):
        @pl.when(i >= KA)
        def _():
            wait_gather(d, i)

        credit(d, n)

        def go(k, l, r):
            pltpu.make_async_remote_copy(
                weight(k, l, dev, r), weight(k, l, dev, r), gsend.at[d, i % KA], recv.at[d, n % SLOTS],
                device_id=nexts[d], device_id_type=MESH).start()

        by_weight(j, go)

    def partner_push(j, dev):
        def go(k, l, r):
            mat = k * LAYERS + l
            pltpu.make_async_remote_copy(
                weight(k, l, dev, r), weight(k, l, dev, r), ag_send.at[mat], ag_recv.at[mat],
                device_id=partner, device_id_type=MESH).start()

        by_weight(j, go)

    def handle(d, t):
        q = qs[d]
        e = t - LAG * q - jnp.where(q == CHIPS - 1, END, 0)
        valid = (e >= 0) & (e < E)
        beta, j = decode(e)
        b = beta if d == 0 else CHIPS - 1 - beta
        dev = 2 * b + c
        s = e % RING

        @pl.when(valid & (q < beta))
        def _():
            wait_local(own.at[d, s], ownsem.at[d, s])
            wait_local(par.at[d, s], parsem.at[d, s])
            i = jnp.where((q == 1) & (beta == 2), NC + j, e)
            o = i % K

            @pl.when(i >= K)
            def _():
                wait_sum(d, i)

            credit(d, e)

            @pl.when(q == 0)
            def _():
                def body(col):
                    total = own[d, s, :, col].astype(jnp.float32) + par[d, s, :, col].astype(jnp.float32)
                    out[d, o, :, col] = total.astype(jnp.bfloat16)

                columns(body)

            @pl.when(q > 0)
            def _():
                wait_recv(d, e)

                def body(col):
                    total = own[d, s, :, col].astype(jnp.float32) + par[d, s, :, col].astype(jnp.float32)
                    out[d, o, :, col] = (total + land[d, e % SLOTS, :, col].astype(jnp.float32)).astype(jnp.bfloat16)

                columns(body)

            pltpu.make_async_remote_copy(
                out.at[d, o], land.at[d, e % SLOTS], send.at[d, o], recv.at[d, e % SLOTS],
                device_id=nexts[d], device_id_type=MESH).start()

        @pl.when(valid & (q == beta) & (beta % 2 == 1))
        def _():
            f = j % FR
            wait_local(own.at[d, s], ownsem.at[d, s])
            wait_local(par.at[d, s], parsem.at[d, s])
            wait_local(mb.at[f], ld_sem.at[0, f])
            wait_local(vb.at[f], ld_sem.at[1, f])
            wait_local(wb.at[f], ld_sem.at[2, f])
            wait_recv(d, e)
            other = NC + jnp.where(j < D, j, 2 * j - D + 1)

            def update(extra, k, l, r):
                for p in range(1 if k < 2 else R):
                    rr = pl.ds(pl.multiple_of((r if k < 2 else r * R + p) * ROWS, ROWS), ROWS)
                    width = C if k < 2 else CD

                    def body(i, _, p=p, rr=rr, width=width):
                        col = pl.ds(pl.multiple_of(p * width + i * CB, CB), CB)
                        to = pl.ds(pl.multiple_of(i * CB, CB), CB)
                        total = own[d, s, :, col].astype(jnp.float32) + par[d, s, :, col].astype(jnp.float32)
                        total = total + land[d, e % SLOTS, :, col].astype(jnp.float32)
                        if extra:
                            total = total + land[1 - d, other % SLOTS, :, col].astype(jnp.float32)
                        grad = total.astype(jnp.bfloat16).astype(jnp.float32)
                        wn[f, :, col], M[k][l, rr, to], V[k][l, rr, to] = adamw(
                            wb[f, :, col].astype(jnp.float32), mb[f, :, col], vb[f, :, col], grad)
                        return 0

                    lax.fori_loop(0, width // CB, body, 0)

            @pl.when(beta == 1)
            def _():
                wait_recv(1 - d, other)
                by_weight(j, functools.partial(update, True))

            @pl.when(beta == 3)
            def _():
                by_weight(j, functools.partial(update, False))

            by_weight(j, lambda k, l, r: save(k, wn.at[f], weight(k, l, me, r), ww_sem))
            wait_local(wn.at[f], ww_sem)

            @pl.when(beta == 1)
            def _():
                gather_send(d, j, dev, j, e)
                gather_send(1 - d, j, dev, 2 * j, NC + 2 * j)

            partner_push(j, dev)
            step_load(j + FR - 1)

        @pl.when(valid & (q == beta) & (beta == 0))
        def _():
            gather_send(d, j, dev, j, e)

        @pl.when(valid & (q == CHIPS - 1) & (beta == 1))
        def _():
            wait_recv(d, NC + 2 * j)
            partner_push(j, dev + jnp.where(d == 0, 2, -2))

        @pl.when(valid & (q > beta) & (beta != 2))
        def _():
            two = beta == 1
            wait_recv(d, jnp.where(two & (q == CHIPS - 1), NC + 2 * j + 1, e))

            @pl.when(q < CHIPS - 1)
            def _():
                i = jnp.where(q == 1, NC + j, jnp.where(two, 2 * j + 1, 2 * NC + j))
                gather_send(d, j, dev, i, jnp.where(two, NC + 2 * j + 1, e))

            partner_push(j, dev)

        done = e - 2 * D

        @pl.when(valid & (q > 0) & (done >= 0) & (done % G == G - 1) & (done < E - SLOTS))
        def _():
            pl.semaphore_signal(credits.at[d], inc=1, device_id=nexts[1 - d], device_id_type=MESH)

        prefetch(d, e + PF)

    barrier = pltpu.get_barrier_semaphore()
    pl.semaphore_signal(barrier, inc=1, device_id=partner, device_id_type=MESH)
    for d in range(2):
        @pl.when(qs[d] < CHIPS - 1)
        def _(d=d):
            pl.semaphore_signal(barrier, inc=1, device_id=nexts[d], device_id_type=MESH)
    for j in range(FR - 1):
        step_load(jnp.int32(j))
    inner = (z > 0) & (z < CHIPS - 1)
    pl.semaphore_wait(barrier, jnp.where(inner, 3, 2))

    def before(i, _):
        pair_push(i)
        return 0

    lax.fori_loop(0, PRE, before, 0)

    def slot(i, _):
        t = i - PF
        pair_push(i + PRE)
        handle(0, t)
        handle(1, t)
        return 0

    lax.fori_loop(0, PF + E + LAG * (CHIPS - 1) + END, slot, 0)

    for d in range(2):
        @pl.when(qs[d] < CHIPS - 1)
        def _(d=d):
            for s in range(K):
                wait_sum(d, s)
            for s in range(KA):
                wait_gather(d, s)
    for s in range(PS):
        pair_wait(d2d_send.at[s])
    for k in range(3):
        half = W[k].shape[1] // 2
        for l in range(LAYERS):
            for sem in (ag_send, ag_recv):
                pltpu.make_async_copy(
                    W[k].at[l, pl.ds(0, half), :], W[k].at[l, pl.ds(0, half), :], sem.at[k * LAYERS + l]).wait()


def place(cuts, *refs):
    src, dst = refs[:9], refs[9:18]
    big, small, held_sem, in_sem, out_sem = refs[18:]
    held = [pltpu.make_async_copy(src[3 + i], dst[3 + i], held_sem.at[i]) for i in range(6)]
    moves = []
    for k in range(3):
        n = src[k].shape[1] // cuts
        for l in range(LAYERS):
            for i in range(cuts):
                s = len(moves) % MOVE
                buf = (big if k < 2 else small).at[s]
                at = (l, pl.ds(i * n, n), slice(None))
                moves.append((pltpu.make_async_copy(src[k].at[at], buf, in_sem.at[s]),
                              pltpu.make_async_copy(buf, dst[k].at[at], out_sem.at[s])))
    ahead = MOVE // 2
    for i in range(len(moves) + ahead):
        if i < len(moves):
            if i >= MOVE:
                moves[i - MOVE][1].wait()
            moves[i][0].start()
        if i == ahead:
            for copy in held:
                copy.start()
        if i >= ahead:
            moves[i - ahead][0].wait()
            moves[i - ahead][1].start()
    for _, out in moves[-MOVE:]:
        out.wait()
    for copy in held:
        copy.wait()


def step(*arrays):
    g, w, m, v = (arrays[i : i + 3] for i in (0, 3, 6, 9))
    C, CD = w[0].shape[2], w[2].shape[2]
    NR = m[0].shape[1] // ROWS
    NC = NR * LAYERS * 3
    CB = 384 if CD % 384 == 0 else CD
    geo = (C, CD, NR, NC, CB)
    E = 4 * NC
    bf, f32 = jnp.bfloat16, jnp.float32
    hbm, vmem = pl.BlockSpec(memory_space=pl.ANY), pl.BlockSpec(memory_space=pltpu.VMEM)
    outs = [jax.ShapeDtypeStruct(x.shape, x.dtype) for x in w]
    outs += [pltpu.VMEM(x.shape, x.dtype) for x in (*m, *v)]
    outs += [jax.ShapeDtypeStruct((LAYERS, CHIPS, *x.shape[1:]), bf) for x in m]
    dma = pltpu.SemaphoreType.DMA
    got = pl.pallas_call(
        functools.partial(kernel, geo),
        out_shape=outs,
        in_specs=[hbm] * 12,
        out_specs=[hbm] * 3 + [vmem] * 6 + [hbm] * 3,
        scratch_shapes=[
            pltpu.VMEM((2, SLOTS, ROWS, C), bf),
            pltpu.VMEM((2, RING, ROWS, C), bf),
            pltpu.VMEM((2, RING, ROWS, C), bf),
            pltpu.VMEM((2, K, ROWS, C), bf),
            pltpu.VMEM((FR, ROWS, C), f32),
            pltpu.VMEM((FR, ROWS, C), f32),
            pltpu.VMEM((FR, ROWS, C), bf),
            pltpu.VMEM((FR, ROWS, C), bf),
            dma((2, SLOTS)),
            pltpu.SemaphoreType.REGULAR((2,)),
            dma((2, K)),
            dma((2, KA)),
            dma((2, RING)),
            dma((2, RING)),
            dma((E // PG,)),
            dma((PS,)),
            dma((3, FR)),
            dma(()),
            dma((3 * LAYERS,)),
            dma((3 * LAYERS,)),
        ],
        compiler_params=pltpu.CompilerParams(collective_id=0, has_side_effects=True, vmem_limit_bytes=20 << 20),
        name="step",
    )(*arrays)
    held = [pltpu.with_memory_space_constraint(x, pltpu.VMEM) for x in got[3:9]]
    big, small = (w[0].shape[1] // 12, C), (w[2].shape[1] // 12, CD)
    return pl.pallas_call(
        functools.partial(place, 12),
        out_shape=[jax.ShapeDtypeStruct(x.shape, x.dtype) for x in (*w, *m, *v)],
        in_specs=[hbm] * 3 + [vmem] * 6,
        out_specs=[hbm] * 9,
        scratch_shapes=[
            pltpu.VMEM((MOVE, *big), bf),
            pltpu.VMEM((MOVE, *small), bf),
            dma((6,)),
            dma((MOVE,)),
            dma((MOVE,)),
        ],
        compiler_params=pltpu.CompilerParams(vmem_limit_bytes=20 << 20),
        name="place",
    )(*got[:3], *held)


def solution(mesh):
    all_of, cut = P(None, None, None), P(None, "dp", None)
    return jax.shard_map(
        step,
        mesh=mesh,
        in_specs=(P(("rep", "dp"), None, None, None),) * 3 + (all_of,) * 3 + (cut,) * 6,
        out_specs=(P("rep", None, None),) * 3 + (P("rep", "dp", None),) * 6,
        check_vma=False,
    )
```

```python
import functools

import jax
import jax.numpy as jnp
from jax import lax
from jax.experimental import pallas as pl
from jax.experimental.pallas import tpu as pltpu
from jax.sharding import PartitionSpec as P


MESH = pl.DeviceIdType.MESH
ROWS = 16
LAYERS = 2
CHIPS = 4
K = 4
KA = 4
LAG = 2
END = 3
D = 2
PF = 2
RING = 3
FR = 2
CUTS = 12
MOVE = 8
U = 4
VMEM_LIMIT = 10 << 20
HELD = 1
PRE = 4
PS = 8
PG = 3
G = 6
SLOTS = 18


def adamw(w, m, v, g):
    m = 0.9 * m + 0.1 * g
    v = 0.95 * v + 0.05 * g * g
    step = m * lax.rsqrt(v + 1e-8) + 0.1 * w
    return (w - 0.02 * step).astype(jnp.bfloat16), m, v


def kernel(geo, *refs):
    C, CD, NR, NC, CB = geo
    R = C // CD
    E = 4 * NC
    g, w, m, v = refs[0:3], refs[3:6], refs[6:9], refs[9:12]
    W, M, V, seed, PT = refs[12:15], refs[15:18], refs[18:21], refs[21], refs[22:25]
    (land, own, par, out, mb, vb, wb, wn, recv, credits, send, gsend, ownsem, parsem, d2d_recv, d2d_send, ld_sem, ww_sem,
     ag_recv, ag_send) = refs[25:]
    rep = lax.axis_index("rep")
    me = lax.axis_index("dp")
    z, c = me // 2, me % 2
    partner = (rep, z * 2 + 1 - c)
    nexts = ((rep, jnp.minimum(z + 1, CHIPS - 1) * 2 + c), (rep, jnp.maximum(z - 1, 0) * 2 + c))
    qs = (z, CHIPS - 1 - z)

    def split(j):
        mat = j // NR
        return mat // LAYERS, mat % LAYERS, j % NR

    def by_weight(j, body):
        k, l, r = split(j)
        for i in range(3):
            @pl.when(k == i)
            def _(i=i):
                body(i, l, r)

    def rows(i, dev, r):
        n = ROWS if i < 2 else ROWS * R
        return pl.ds(pl.multiple_of((dev * NR + r) * n, n), n)

    def load(i, src, dst, sem):
        if i < 2:
            pltpu.make_async_copy(src, dst, sem).start()
        else:
            for s in range(R):
                pltpu.make_async_copy(src.at[pl.ds(s * ROWS, ROWS), :], dst.at[:, pl.ds(s * CD, CD)], sem).start()

    def save(i, src, dst, sem):
        if i < 2:
            pltpu.make_async_copy(src, dst, sem).start()
        else:
            for s in range(R):
                pltpu.make_async_copy(src.at[:, pl.ds(s * CD, CD)], dst.at[pl.ds(s * ROWS, ROWS), :], sem).start()

    def wait_local(buf, sem):
        pltpu.make_async_copy(buf, buf, sem).wait()

    def decode(e):
        p = e - NC
        x = p - D
        first, last, head, tail = p < 0, p >= 2 * NC, p < D, p >= 2 * NC - D
        beta = jnp.where(first, 3, jnp.where(last, 0, jnp.where(head, 2, jnp.where(tail, 1, 1 + x % 2))))
        mid = jnp.where(x % 2 == 0, x // 2, D + x // 2)
        j = jnp.where(first, e, jnp.where(last, p - 2 * NC, jnp.where(head, p, jnp.where(tail, p - NC, mid))))
        return beta, j

    def sums(e, q):
        beta, j = decode(e)
        return (e >= 0) & (e < E) & ((q < beta) | ((q == beta) & (beta % 2 == 1))), beta, j

    def pair_index(b, i):
        n = NC // PG
        return jnp.where((b == 0) | (b == 3), 2 * i + jnp.where(b == 0, 1, 0), 2 * n + 2 * i + jnp.where(b == 1, 1, 0))

    def pair_group(i):
        n = NC // PG
        late = i >= 2 * n
        odd = i % 2
        b = jnp.where(late, 2 - odd, 3 - 3 * odd)
        return b, jnp.where(late, i - 2 * n, i) // 2

    def pair_wait(sem):
        many = land.at[0, pl.ds(0, PG)]
        pltpu.make_async_copy(many, many, sem).wait()

    def pair_push(i):
        @pl.when(i < 4 * NC // PG)
        def _():
            @pl.when(i >= PS)
            def _():
                pair_wait(d2d_send.at[i % PS])

            b, group = pair_group(i)

            def go(k, l, r):
                n = (ROWS if k < 2 else ROWS * R) * PG
                src = pl.ds(pl.multiple_of(((2 * b + 1 - c) * NR + r) * (n // PG), n), n)
                dst = pl.ds(pl.multiple_of(r * (n // PG), n), n)
                pltpu.make_async_remote_copy(
                    g[k].at[0, l, src, :], PT[k].at[l, b, dst, :], d2d_send.at[i % PS], d2d_recv.at[i],
                    device_id=partner, device_id_type=MESH).start()

            by_weight(group * PG, go)

    def prefetch(d, e):
        need, beta, j = sums(e, qs[d])
        b = beta if d == 0 else CHIPS - 1 - beta

        @pl.when(need)
        def _():
            s = e % RING
            by_weight(j, lambda k, l, r: load(k, g[k].at[0, l, rows(k, 2 * b + c, r), :], own.at[d, s], ownsem.at[d, s]))

            @pl.when(j % PG == 0)
            def _():
                pair_wait(d2d_recv.at[pair_index(b, j // PG)])

            by_weight(j, lambda k, l, r: load(k, PT[k].at[l, b, rows(k, 0, r), :], par.at[d, s], parsem.at[d, s]))

    def step_load(j):
        @pl.when(j < NC)
        def _():
            s = j % FR

            def go(k, l, r):
                load(k, m[k].at[l, rows(k, 0, r), :], mb.at[s], ld_sem.at[0, s])
                load(k, v[k].at[l, rows(k, 0, r), :], vb.at[s], ld_sem.at[1, s])
                load(k, w[k].at[l, rows(k, me, r), :], wb.at[s], ld_sem.at[2, s])

            by_weight(j, go)

    def wait_sum(d, n):
        pltpu.make_async_copy(out.at[d, 0], out.at[d, 0], send.at[d, n % K]).wait()

    def wait_gather(d, n):
        pltpu.make_async_copy(out.at[d, 0], out.at[d, 0], gsend.at[d, n % KA]).wait()

    def wait_recv(d, n):
        pltpu.make_async_copy(land.at[d, 0], land.at[d, 0], recv.at[d, n % SLOTS]).wait()

    def credit(d, n):
        @pl.when((n >= SLOTS) & (n % G == 0))
        def _():
            pl.semaphore_wait(credits.at[d], 1)

    def columns(body):
        def step(i, _):
            body(pl.ds(pl.multiple_of(i * CB, CB), CB))
            return 0

        lax.fori_loop(0, C // CB, step, 0)

    def weight(k, l, dev, r):
        return W[k].at[l, rows(k, dev, r), :]

    def gather_send(d, j, dev, i, n):
        @pl.when(i >= KA)
        def _():
            wait_gather(d, i)

        credit(d, n)

        def go(k, l, r):
            pltpu.make_async_remote_copy(
                weight(k, l, dev, r), weight(k, l, dev, r), gsend.at[d, i % KA], recv.at[d, n % SLOTS],
                device_id=nexts[d], device_id_type=MESH).start()

        by_weight(j, go)

    def partner_push(j, dev):
        def go(k, l, r):
            mat = k * LAYERS + l
            pltpu.make_async_remote_copy(
                weight(k, l, dev, r), weight(k, l, dev, r), ag_send.at[mat], ag_recv.at[mat],
                device_id=partner, device_id_type=MESH).start()

        by_weight(j, go)

    def handle(d, t):
        q = qs[d]
        e = t - LAG * q - jnp.where(q == CHIPS - 1, END, 0)
        sent = NC - (q + 1) * U
        came = jnp.where(q == 0, sent, sent + U)
        valid = (e >= 0) & (e < 3 * NC + came)
        beta, j = decode(e)
        b = beta if d == 0 else CHIPS - 1 - beta
        dev = 2 * b + c
        s = e % RING

        @pl.when(valid & (q < beta))
        def _():
            wait_local(own.at[d, s], ownsem.at[d, s])
            wait_local(par.at[d, s], parsem.at[d, s])
            i = jnp.where((q == 1) & (beta == 2), NC + j, e)
            o = i % K

            @pl.when(i >= K)
            def _():
                wait_sum(d, i)

            credit(d, e)

            @pl.when(q == 0)
            def _():
                def body(col):
                    total = own[d, s, :, col].astype(jnp.float32) + par[d, s, :, col].astype(jnp.float32)
                    out[d, o, :, col] = total.astype(jnp.bfloat16)

                columns(body)

            @pl.when(q > 0)
            def _():
                wait_recv(d, e)

                def body(col):
                    total = own[d, s, :, col].astype(jnp.float32) + par[d, s, :, col].astype(jnp.float32)
                    out[d, o, :, col] = (total + land[d, e % SLOTS, :, col].astype(jnp.float32)).astype(jnp.bfloat16)

                columns(body)

            pltpu.make_async_remote_copy(
                out.at[d, o], land.at[d, e % SLOTS], send.at[d, o], recv.at[d, e % SLOTS],
                device_id=nexts[d], device_id_type=MESH).start()

        @pl.when(valid & (q == beta) & (beta % 2 == 1))
        def _():
            f = j % FR
            wait_local(own.at[d, s], ownsem.at[d, s])
            wait_local(par.at[d, s], parsem.at[d, s])
            wait_local(mb.at[f], ld_sem.at[0, f])
            wait_local(vb.at[f], ld_sem.at[1, f])
            wait_local(wb.at[f], ld_sem.at[2, f])
            wait_recv(d, e)
            other = NC + jnp.where(j < D, j, 2 * j - D + 1)

            def update(extra, k, l, r):
                for p in range(1 if k < 2 else R):
                    rr = pl.ds(pl.multiple_of((r if k < 2 else r * R + p) * ROWS, ROWS), ROWS)
                    width = C if k < 2 else CD

                    def body(i, _, p=p, rr=rr, width=width):
                        col = pl.ds(pl.multiple_of(p * width + i * CB, CB), CB)
                        to = pl.ds(pl.multiple_of(i * CB, CB), CB)
                        total = own[d, s, :, col].astype(jnp.float32) + par[d, s, :, col].astype(jnp.float32)
                        total = total + land[d, e % SLOTS, :, col].astype(jnp.float32)
                        if extra:
                            total = total + land[1 - d, other % SLOTS, :, col].astype(jnp.float32)
                        grad = total.astype(jnp.bfloat16).astype(jnp.float32)
                        new, M[k][l, rr, to], V[k][l, rr, to] = adamw(
                            wb[f, :, col].astype(jnp.float32), mb[f, :, col], vb[f, :, col], grad)
                        if k < HELD:
                            W[k][l, rows(k, me, r), to] = new
                        else:
                            wn[f, :, col] = new
                        return 0

                    lax.fori_loop(0, width // CB, body, 0)

            @pl.when(beta == 1)
            def _():
                wait_recv(1 - d, other)
                by_weight(j, functools.partial(update, True))

            @pl.when(beta == 3)
            def _():
                by_weight(j, functools.partial(update, False))

            def put(k, l, r):
                if k >= HELD:
                    save(k, wn.at[f], weight(k, l, me, r), ww_sem)
                    wait_local(wn.at[f], ww_sem)

            by_weight(j, put)

            @pl.when(beta == 1)
            def _():
                gather_send(d, j, dev, j, e)
                gather_send(1 - d, j, dev, 2 * j, NC + 2 * j)

            partner_push(j, dev)
            step_load(j + FR - 1)

        @pl.when(valid & (q == beta) & (beta == 0))
        def _():
            gather_send(d, j, dev, j, e)

        @pl.when(valid & (q == CHIPS - 1) & (beta == 1))
        def _():
            wait_recv(d, NC + 2 * j)
            partner_push(j, dev + jnp.where(d == 0, 2, -2))

        @pl.when(valid & (q > beta) & (beta != 2))
        def _():
            two = beta == 1
            wait_recv(d, jnp.where(two & (q == CHIPS - 1), NC + 2 * j + 1, e))

            @pl.when((q < CHIPS - 1) & ((beta > 0) | (j < sent)))
            def _():
                i = jnp.where(q == 1, NC + j, jnp.where(two, 2 * j + 1, 2 * NC + j))
                gather_send(d, j, dev, i, jnp.where(two, NC + 2 * j + 1, e))

            partner_push(j, dev)

        done = e - 2 * D

        @pl.when(valid & (q > 0) & (done >= 0) & (done % G == G - 1) & (done + 1 - G + SLOTS < 3 * NC + came))
        def _():
            pl.semaphore_signal(credits.at[d], inc=1, device_id=nexts[1 - d], device_id_type=MESH)

        prefetch(d, e + PF)

    barrier = pltpu.get_barrier_semaphore()
    pl.semaphore_signal(barrier, inc=1, device_id=partner, device_id_type=MESH)
    for d in range(2):
        @pl.when(qs[d] < CHIPS - 1)
        def _(d=d):
            pl.semaphore_signal(barrier, inc=1, device_id=nexts[d], device_id_type=MESH)
    for j in range(FR - 1):
        step_load(jnp.int32(j))
    inner = (z > 0) & (z < CHIPS - 1)
    pl.semaphore_wait(barrier, jnp.where(inner, 3, 2))

    def before(i, _):
        pair_push(i)
        return 0

    lax.fori_loop(0, PRE, before, 0)

    def slot(i, _):
        t = i - PF
        pair_push(i + PRE)
        handle(0, t)
        handle(1, t)
        return 0

    lax.fori_loop(0, PF + E + LAG * (CHIPS - 1) + END, slot, 0)

    for d in range(2):
        @pl.when(qs[d] < CHIPS - 1)
        def _(d=d):
            for s in range(K):
                wait_sum(d, s)
            for s in range(KA):
                wait_gather(d, s)
    for s in range(PS):
        pair_wait(d2d_send.at[s])

    def pushed(k, l, chunks):
        if chunks:
            n = chunks * (ROWS if k < 2 else ROWS * R)
            for sem in (ag_send, ag_recv):
                pltpu.make_async_copy(W[k].at[l, pl.ds(0, n), :], W[k].at[l, pl.ds(0, n), :], sem.at[k * LAYERS + l]).wait()

    for k in range(2):
        for l in range(LAYERS):
            pushed(k, l, CHIPS * NR)
    for at in range(CHIPS):
        @pl.when(z == at)
        def _(at=at):
            for l in range(LAYERS):
                start = (2 * LAYERS + l) * NR
                here = [NC - far * U for far in (at, CHIPS - 1 - at)]
                pushed(2, l, 2 * NR + sum(min(max(n - start, 0), NR) for n in here))

    for d in range(2):
        @pl.when((c == d) & (qs[d] < CHIPS - 1))
        def _(d=d):
            for lane in range(2):
                for i in range(U):
                    _, l, r = split(NC - (qs[d] + 1) * U + i)
                    block = (0 if d == 0 else CHIPS - 1) * 2 + lane
                    pltpu.make_async_copy(weight(2, l, block, r), seed.at[lane * U + i], ww_sem).start()
            wait_local(seed, ww_sem)


def place_held(*refs):
    n = len(refs) // 2
    for i in range(n):
        parts = 4 if i < HELD else 1
        rows = refs[i].shape[1] // parts
        for l in range(LAYERS):
            for p in range(parts):
                at = (l, pl.ds(p * rows, rows), slice(None))
                pltpu.make_async_copy(refs[i].at[at], refs[n + i].at[at], refs[-1].at[i]).start()
    for i in range(n):
        pltpu.make_async_copy(refs[i], refs[n + i], refs[-1].at[i]).wait()


def place(cuts, src, dst, ring, in_sem, out_sem):
    n = src.shape[1] // cuts
    moves = []
    for l in range(LAYERS):
        for i in range(cuts):
            at, s = (l, pl.ds(i * n, n), slice(None)), len(moves) % MOVE
            moves.append((pltpu.make_async_copy(src.at[at], ring.at[s], in_sem.at[s]),
                          pltpu.make_async_copy(ring.at[s], dst.at[at], out_sem.at[s])))
    ahead = MOVE // 2
    for i in range(len(moves) + ahead):
        if i < len(moves):
            if i >= MOVE:
                moves[i - MOVE][1].wait()
            moves[i][0].start()
        if i >= ahead:
            moves[i - ahead][0].wait()
            moves[i - ahead][1].start()
    for _, out in moves[-MOVE:]:
        out.wait()


def fill(geo, rounds, old, *refs):
    C, CD, NR, NC, _ = geo
    R = C // CD
    n = len(rounds)
    got, swapped, new, sem = refs[:n], refs[n : 2 * n], refs[2 * n], refs[2 * n + 1]
    me = lax.axis_index("dp")
    z, c = me // 2, me % 2
    qs = (z, CHIPS - 1 - z)
    h = ROWS * R

    def each(body):
        for a, r in enumerate(rounds):
            for d in range(2):
                @pl.when(qs[d] >= r)
                def _(a=a, r=r, d=d):
                    body(a, r, d, sem.at[a * 2 + d])

    def put(a, r, d, sem):
        for lane in range(2):
            for i in range(U):
                j = NC - qs[d] * U + (r - 1) * U + i - 2 * LAYERS * NR
                block = (0 if d == 0 else CHIPS - 1) * 2 + lane
                to = new.at[j // NR, pl.ds(pl.multiple_of((block * NR + j % NR) * h, h), h), :]
                for mine, src in ((True, got[a]), (False, swapped[a])):
                    @pl.when((c == d) == mine)
                    def _(src=src, to=to, lane=lane, i=i):
                        pltpu.make_async_copy(src.at[lane * U + i], to, sem).start()

    def end(a, r, d, sem):
        pltpu.make_async_copy(got[a], got[a], sem).wait()

    each(put)
    each(end)


def step(*arrays):
    _, w, m, v = (arrays[i : i + 3] for i in (0, 3, 6, 9))
    C, CD = w[0].shape[2], w[2].shape[2]
    NR = m[0].shape[1] // ROWS
    NC = NR * LAYERS * 3
    CB = 384 if CD % 384 == 0 else CD
    geo = (C, CD, NR, NC, CB)
    E = 4 * NC
    bf, f32 = jnp.bfloat16, jnp.float32
    hbm, vmem = pl.BlockSpec(memory_space=pl.ANY), pl.BlockSpec(memory_space=pltpu.VMEM)
    outs = [pltpu.VMEM(x.shape, x.dtype) for x in w[:HELD]] + [jax.ShapeDtypeStruct(x.shape, x.dtype) for x in w[HELD:]]
    outs += [pltpu.VMEM(x.shape, x.dtype) for x in (*m, *v)]
    piece = (2 * U, ROWS * (C // CD), CD)
    outs += [pltpu.VMEM(piece, bf)]
    outs += [jax.ShapeDtypeStruct((LAYERS, CHIPS, *x.shape[1:]), bf) for x in m]
    dma = pltpu.SemaphoreType.DMA
    got = pl.pallas_call(
        functools.partial(kernel, geo),
        out_shape=outs,
        in_specs=[hbm] * 12,
        out_specs=[vmem] * HELD + [hbm] * (3 - HELD) + [vmem] * 7 + [hbm] * 3,
        scratch_shapes=[
            pltpu.VMEM((2, SLOTS, ROWS, C), bf),
            pltpu.VMEM((2, RING, ROWS, C), bf),
            pltpu.VMEM((2, RING, ROWS, C), bf),
            pltpu.VMEM((2, K, ROWS, C), bf),
            pltpu.VMEM((FR, ROWS, C), f32),
            pltpu.VMEM((FR, ROWS, C), f32),
            pltpu.VMEM((FR, ROWS, C), bf),
            pltpu.VMEM((FR, ROWS, C), bf),
            dma((2, SLOTS)),
            pltpu.SemaphoreType.REGULAR((2,)),
            dma((2, K)),
            dma((2, KA)),
            dma((2, RING)),
            dma((2, RING)),
            dma((E // PG,)),
            dma((PS,)),
            dma((3, FR)),
            dma(()),
            dma((3 * LAYERS,)),
            dma((3 * LAYERS,)),
        ],
        compiler_params=pltpu.CompilerParams(collective_id=0, has_side_effects=True, vmem_limit_bytes=VMEM_LIMIT),
        name="step",
    )(*arrays)
    seed = got[9]
    in_vmem = [pltpu.with_memory_space_constraint(got[i], pltpu.VMEM) for i in (*range(HELD), *range(3, 9))]
    local = pltpu.CompilerParams(vmem_limit_bytes=VMEM_LIMIT)

    def onward(first):
        there = [(2 * p, 2 * p + 2) for p in range(first, CHIPS - 1)]
        return there + [(2 * CHIPS - 1 - a, 2 * CHIPS - 1 - b) for a, b in there]

    got_by, swapped = [], []
    for r in range(CHIPS - 1):
        seed = lax.ppermute(seed, "dp", onward(r))
        got_by.append(pltpu.with_memory_space_constraint(seed, pltpu.VMEM))
        other = lax.ppermute(seed, "dp", [(i, i ^ 1) for i in range(2 * CHIPS)])
        swapped.append(pltpu.with_memory_space_constraint(other, pltpu.VMEM))

    def cost(n):
        return pl.CostEstimate(flops=n, bytes_accessed=n, transcendentals=0)

    def move(k):
        shape = w[k].shape
        return pl.pallas_call(
            functools.partial(place, CUTS),
            out_shape=jax.ShapeDtypeStruct(shape, bf),
            in_specs=[hbm],
            out_specs=hbm,
            scratch_shapes=[pltpu.VMEM((MOVE, shape[1] // CUTS, shape[2]), bf), dma((MOVE,)), dma((MOVE,))],
            compiler_params=local,
            cost_estimate=cost(4 * w[k].size),
        )(pltpu.with_memory_space_constraint(got[k], pltpu.HBM))

    def take(rounds, old):
        n = len(rounds)
        return pl.pallas_call(
            functools.partial(fill, geo, rounds),
            out_shape=jax.ShapeDtypeStruct(old.shape, bf),
            in_specs=[hbm] + [vmem] * (2 * n),
            out_specs=hbm,
            scratch_shapes=[dma((2 * n,))],
            input_output_aliases={0: 0},
            compiler_params=local,
            cost_estimate=cost(4 * n * 6 * U * 1000),
        )(old, *(got_by[r - 1] for r in rounds), *(swapped[r - 1] for r in rounds))

    shapes = [x.shape for x in w[:HELD]] + [x.shape for x in (*m, *v)]
    types = [bf] * HELD + [f32] * 6
    placed = pl.pallas_call(
        place_held,
        out_shape=[jax.ShapeDtypeStruct(a, b) for a, b in zip(shapes, types, strict=True)],
        in_specs=[vmem] * len(in_vmem),
        out_specs=[hbm] * len(in_vmem),
        scratch_shapes=[dma((len(in_vmem),))],
        compiler_params=local,
        cost_estimate=cost(8 * w[0].size),
        name="place_held",
    )(*in_vmem)
    up = move(1)
    down = move(2)
    down = take((1, 2), down)
    down = take((3,), down)
    return (placed[0], up, down, *placed[1:])


def solution(mesh):
    all_of, cut = P(None, None, None), P(None, "dp", None)

    return jax.shard_map(
        step,
        mesh=mesh,
        in_specs=(P(("rep", "dp"), None, None, None),) * 3 + (all_of,) * 3 + (cut,) * 6,
        out_specs=(P("rep", None, None),) * 3 + (P("rep", "dp", None),) * 6,
        check_vma=False,
    )
```

```python
import functools

import jax
import jax.numpy as jnp
from jax import lax
from jax.experimental import pallas as pl
from jax.experimental.pallas import tpu as pltpu
from jax.sharding import PartitionSpec as P


MESH = pl.DeviceIdType.MESH
ROWS = 16
LAYERS = 2
CHIPS = 4
K = 4
KA = 4
LAG = 2
END = 3
D = 2
PF = 2
RING = 3
FR = 2
CUTS = 24
MOVE = 8
U = 4
HOPS = CHIPS - 1
VMEM_LIMIT = 10 << 20
HELD = 1
PRE = 4
PS = 8
PG = 9
G = 6
SLOTS = 18


def adamw(w, m, v, g):
    m = 0.9 * m + 0.1 * g
    v = 0.95 * v + 0.05 * g * g
    step = m * lax.rsqrt(v + 1e-8) + 0.1 * w
    return (w - 0.02 * step).astype(jnp.bfloat16), m, v


def kernel(geo, *refs):
    C, CD, NR, NC, CB = geo
    R = C // CD
    E = 4 * NC
    g, w, m, v = refs[0:3], refs[3:6], refs[6:9], refs[9:12]
    W, M, V, seed, PT = refs[12:15], refs[15:18], refs[18:21], refs[21], refs[22:25]
    (land, own, par, out, mb, vb, wb, wn, recv, credits, send, gsend, ownsem, parsem, d2d_recv, d2d_send, d2d_first, ld_sem, ww_sem,
     ag_recv, ag_send, seed_sem) = refs[25:]
    rep = lax.axis_index("rep")
    me = lax.axis_index("dp")
    z, c = me // 2, me % 2
    partner = (rep, z * 2 + 1 - c)
    nexts = ((rep, jnp.minimum(z + 1, CHIPS - 1) * 2 + c), (rep, jnp.maximum(z - 1, 0) * 2 + c))
    qs = (z, CHIPS - 1 - z)

    def split(j):
        mat = j // NR
        return mat // LAYERS, mat % LAYERS, j % NR

    def by_weight(j, body):
        k, l, r = split(j)
        for i in range(3):
            @pl.when(k == i)
            def _(i=i):
                body(i, l, r)

    def rows(i, dev, r):
        n = ROWS if i < 2 else ROWS * R
        return pl.ds(pl.multiple_of((dev * NR + r) * n, n), n)

    def load(i, src, dst, sem):
        if i < 2:
            pltpu.make_async_copy(src, dst, sem).start()
        else:
            for s in range(R):
                pltpu.make_async_copy(src.at[pl.ds(s * ROWS, ROWS), :], dst.at[:, pl.ds(s * CD, CD)], sem).start()

    def save(i, src, dst, sem):
        if i < 2:
            pltpu.make_async_copy(src, dst, sem).start()
        else:
            for s in range(R):
                pltpu.make_async_copy(src.at[:, pl.ds(s * CD, CD)], dst.at[pl.ds(s * ROWS, ROWS), :], sem).start()

    def wait_local(buf, sem):
        pltpu.make_async_copy(buf, buf, sem).wait()

    def decode(e):
        p = e - NC
        x = p - D
        first, last, head, tail = p < 0, p >= 2 * NC, p < D, p >= 2 * NC - D
        beta = jnp.where(first, 3, jnp.where(last, 0, jnp.where(head, 2, jnp.where(tail, 1, 1 + x % 2))))
        mid = jnp.where(x % 2 == 0, x // 2, D + x // 2)
        j = jnp.where(first, e, jnp.where(last, p - 2 * NC, jnp.where(head, p, jnp.where(tail, p - NC, mid))))
        return beta, j

    def sums(e, q):
        beta, j = decode(e)
        return (e >= 0) & (e < E) & ((q < beta) | ((q == beta) & (beta % 2 == 1))), beta, j

    def pair_index(b, i):
        n = NC // PG
        return jnp.where((b == 0) | (b == 3), 2 * i + jnp.where(b == 0, 1, 0), 2 * n + 2 * i + jnp.where(b == 1, 1, 0))

    def pair_group(i):
        n = NC // PG
        late = i >= 2 * n
        odd = i % 2
        b = jnp.where(late, 2 - odd, 3 - 3 * odd)
        return b, jnp.where(late, i - 2 * n, i) // 2

    def pair_wait(sem):
        many = land.at[0, pl.ds(0, PG)]
        pltpu.make_async_copy(many, many, sem).wait()

    def pair_push(i):
        @pl.when(i < 4 * NC // PG)
        def _():
            @pl.when(i >= PS)
            def _():
                pair_wait(d2d_send.at[i % PS])

            b, group = pair_group(i)

            def go(k, l, r):
                n = (ROWS if k < 2 else ROWS * R) * PG
                src = pl.ds(pl.multiple_of(((2 * b + 1 - c) * NR + r) * (n // PG), n), n)
                dst = pl.ds(pl.multiple_of(r * (n // PG), n), n)
                pltpu.make_async_remote_copy(
                    g[k].at[0, l, src, :], PT[k].at[l, b, dst, :], d2d_send.at[i % PS], d2d_recv.at[i],
                    device_id=partner, device_id_type=MESH).start()

            by_weight(group * PG, go)

    def first_push(d, e):
        b = (CHIPS - 1) * (1 - d)
        pltpu.make_async_remote_copy(
            g[0].at[0, 0, rows(0, 2 * b + 1 - c, e), :], par.at[d, e], d2d_first.at[d, e], parsem.at[d, e],
            device_id=partner, device_id_type=MESH).start()

    def prefetch(d, e):
        need, beta, j = sums(e, qs[d])
        b = beta if d == 0 else CHIPS - 1 - beta

        @pl.when(need)
        def _():
            s = e % RING
            by_weight(j, lambda k, l, r: load(k, g[k].at[0, l, rows(k, 2 * b + c, r), :], own.at[d, s], ownsem.at[d, s]))

            @pl.when((j % PG == 0) & (e >= RING) | (e == RING))
            def _():
                pair_wait(d2d_recv.at[pair_index(b, j // PG)])

            @pl.when(e >= RING)
            def _():
                by_weight(j, lambda k, l, r: load(k, PT[k].at[l, b, rows(k, 0, r), :], par.at[d, s], parsem.at[d, s]))

    def step_load(j):
        @pl.when(j < NC)
        def _():
            s = j % FR

            def go(k, l, r):
                load(k, m[k].at[l, rows(k, 0, r), :], mb.at[s], ld_sem.at[0, s])
                load(k, v[k].at[l, rows(k, 0, r), :], vb.at[s], ld_sem.at[1, s])
                load(k, w[k].at[l, rows(k, me, r), :], wb.at[s], ld_sem.at[2, s])

            by_weight(j, go)

    def wait_sum(d, n):
        pltpu.make_async_copy(out.at[d, 0], out.at[d, 0], send.at[d, n % K]).wait()

    def wait_gather(d, n):
        pltpu.make_async_copy(out.at[d, 0], out.at[d, 0], gsend.at[d, n % KA]).wait()

    def wait_recv(d, n):
        pltpu.make_async_copy(land.at[d, 0], land.at[d, 0], recv.at[d, n % SLOTS]).wait()

    def credit(d, n):
        @pl.when((n >= SLOTS) & (n % G == 0))
        def _():
            pl.semaphore_wait(credits.at[d], 1)

    def columns(body):
        def step(i, _):
            body(pl.ds(pl.multiple_of(i * CB, CB), CB))
            return 0

        lax.fori_loop(0, C // CB, step, 0)

    def weight(k, l, dev, r):
        return W[k].at[l, rows(k, dev, r), :]

    def gather_send(d, j, dev, i, n):
        @pl.when(i >= KA)
        def _():
            wait_gather(d, i)

        credit(d, n)

        def go(k, l, r):
            pltpu.make_async_remote_copy(
                weight(k, l, dev, r), weight(k, l, dev, r), gsend.at[d, i % KA], recv.at[d, n % SLOTS],
                device_id=nexts[d], device_id_type=MESH).start()

        by_weight(j, go)

    def partner_push(j, dev):
        def go(k, l, r):
            mat = k * LAYERS + l
            pltpu.make_async_remote_copy(
                weight(k, l, dev, r), weight(k, l, dev, r), ag_send.at[mat], ag_recv.at[mat],
                device_id=partner, device_id_type=MESH).start()

        by_weight(j, go)

    def handle(d, t):
        q = qs[d]
        e = t - LAG * q - jnp.where(q == CHIPS - 1, END, 0)
        sent = NC - (q + 1) * U
        came = jnp.where(q == 0, sent, sent + U)
        valid = (e >= 0) & (e < 3 * NC + came)
        beta, j = decode(e)
        b = beta if d == 0 else CHIPS - 1 - beta
        dev = 2 * b + c
        s = e % RING

        @pl.when(valid & (q < beta))
        def _():
            wait_local(own.at[d, s], ownsem.at[d, s])
            wait_local(par.at[d, s], parsem.at[d, s])
            i = jnp.where((q == 1) & (beta == 2), NC + j, e)
            o = i % K

            @pl.when(i >= K)
            def _():
                wait_sum(d, i)

            credit(d, e)

            @pl.when(q == 0)
            def _():
                def body(col):
                    total = own[d, s, :, col].astype(jnp.float32) + par[d, s, :, col].astype(jnp.float32)
                    out[d, o, :, col] = total.astype(jnp.bfloat16)

                columns(body)

            @pl.when(q > 0)
            def _():
                wait_recv(d, e)

                def body(col):
                    total = own[d, s, :, col].astype(jnp.float32) + par[d, s, :, col].astype(jnp.float32)
                    out[d, o, :, col] = (total + land[d, e % SLOTS, :, col].astype(jnp.float32)).astype(jnp.bfloat16)

                columns(body)

            pltpu.make_async_remote_copy(
                out.at[d, o], land.at[d, e % SLOTS], send.at[d, o], recv.at[d, e % SLOTS],
                device_id=nexts[d], device_id_type=MESH).start()

        @pl.when(valid & (q == beta) & (beta % 2 == 1))
        def _():
            f = j % FR
            wait_local(own.at[d, s], ownsem.at[d, s])
            wait_local(par.at[d, s], parsem.at[d, s])
            wait_local(mb.at[f], ld_sem.at[0, f])
            wait_local(vb.at[f], ld_sem.at[1, f])
            wait_local(wb.at[f], ld_sem.at[2, f])
            wait_recv(d, e)
            other = NC + jnp.where(j < D, j, 2 * j - D + 1)

            def update(extra, k, l, r):
                for p in range(1 if k < 2 else R):
                    rr = pl.ds(pl.multiple_of((r if k < 2 else r * R + p) * ROWS, ROWS), ROWS)
                    width = C if k < 2 else CD

                    def body(i, _, p=p, rr=rr, width=width):
                        col = pl.ds(pl.multiple_of(p * width + i * CB, CB), CB)
                        to = pl.ds(pl.multiple_of(i * CB, CB), CB)
                        total = own[d, s, :, col].astype(jnp.float32) + par[d, s, :, col].astype(jnp.float32)
                        total = total + land[d, e % SLOTS, :, col].astype(jnp.float32)
                        if extra:
                            total = total + land[1 - d, other % SLOTS, :, col].astype(jnp.float32)
                        grad = total.astype(jnp.bfloat16).astype(jnp.float32)
                        new, M[k][l, rr, to], V[k][l, rr, to] = adamw(
                            wb[f, :, col].astype(jnp.float32), mb[f, :, col], vb[f, :, col], grad)
                        if k < HELD:
                            W[k][l, rows(k, me, r), to] = new
                        else:
                            wn[f, :, col] = new
                        return 0

                    lax.fori_loop(0, width // CB, body, 0)

            @pl.when(beta == 1)
            def _():
                wait_recv(1 - d, other)
                by_weight(j, functools.partial(update, True))

            @pl.when(beta == 3)
            def _():
                by_weight(j, functools.partial(update, False))

            def put(k, l, r):
                if k >= HELD:
                    save(k, wn.at[f], weight(k, l, me, r), ww_sem)
                    wait_local(wn.at[f], ww_sem)

            by_weight(j, put)

            @pl.when(beta == 1)
            def _():
                gather_send(d, j, dev, j, e)
                gather_send(1 - d, j, dev, 2 * j, NC + 2 * j)

            partner_push(j, dev)
            step_load(j + FR - 1)

        @pl.when(valid & (q == beta) & (beta == 0))
        def _():
            gather_send(d, j, dev, j, e)

        @pl.when(valid & (q == CHIPS - 1) & (beta == 1))
        def _():
            wait_recv(d, NC + 2 * j)
            partner_push(j, dev + jnp.where(d == 0, 2, -2))

        @pl.when(valid & (q > beta) & (beta != 2))
        def _():
            two = beta == 1
            wait_recv(d, jnp.where(two & (q == CHIPS - 1), NC + 2 * j + 1, e))

            @pl.when((q < CHIPS - 1) & ((beta > 0) | (j < sent)))
            def _():
                i = jnp.where(q == 1, NC + j, jnp.where(two, 2 * j + 1, 2 * NC + j))
                gather_send(d, j, dev, i, jnp.where(two, NC + 2 * j + 1, e))

            partner_push(j, dev)

        i = jnp.where(q == 0, j, j - sent)

        @pl.when(valid & (beta == 0) & (q < CHIPS - 1) & (i >= 0) & (i < U))
        def _():
            _, l, r = split(sent + i)
            src, dst = weight(2, l, dev, r), seed.at[c * U + i]

            @pl.when(c == d)
            def _():
                pltpu.make_async_copy(src, dst, seed_sem.at[0]).start()

            @pl.when(c != d)
            def _():
                pltpu.make_async_remote_copy(
                    src, dst, seed_sem.at[1], seed_sem.at[2], device_id=partner, device_id_type=MESH).start()

        done = e - 2 * D

        @pl.when(valid & (q > 0) & (done >= 0) & (done % G == G - 1) & (done + 1 - G + SLOTS < 3 * NC + came))
        def _():
            pl.semaphore_signal(credits.at[d], inc=1, device_id=nexts[1 - d], device_id_type=MESH)

        prefetch(d, e + PF)

    barrier = pltpu.get_barrier_semaphore()
    pl.semaphore_signal(barrier, inc=1, device_id=partner, device_id_type=MESH)
    for d in range(2):
        @pl.when(qs[d] < CHIPS - 1)
        def _(d=d):
            pl.semaphore_signal(barrier, inc=1, device_id=nexts[d], device_id_type=MESH)
    for j in range(FR - 1):
        step_load(jnp.int32(j))
    inner = (z > 0) & (z < CHIPS - 1)
    pl.semaphore_wait(barrier, jnp.where(inner, 3, 2))

    def before(i, _):
        pair_push(i)
        return 0

    for e in range(RING):
        for d in range(2):
            first_push(d, e)
    lax.fori_loop(0, PRE, before, 0)

    def slot(i, _):
        t = i - PF
        pair_push(i + PRE)
        handle(0, t)
        handle(1, t)
        return 0

    lax.fori_loop(0, PF + E + LAG * (CHIPS - 1) + END, slot, 0)

    for d in range(2):
        @pl.when(qs[d] < CHIPS - 1)
        def _(d=d):
            for s in range(K):
                wait_sum(d, s)
            for s in range(KA):
                wait_gather(d, s)
    for s in range(PS):
        pair_wait(d2d_send.at[s])
    for e in range(RING):
        for d in range(2):
            wait_local(par.at[d, e], d2d_first.at[d, e])

    def pushed(k, l, chunks):
        if chunks:
            n = chunks * (ROWS if k < 2 else ROWS * R)
            for sem in (ag_send, ag_recv):
                pltpu.make_async_copy(W[k].at[l, pl.ds(0, n), :], W[k].at[l, pl.ds(0, n), :], sem.at[k * LAYERS + l]).wait()

    for k in range(2):
        for l in range(LAYERS):
            pushed(k, l, CHIPS * NR)
    for at in range(CHIPS):
        @pl.when(z == at)
        def _(at=at):
            for l in range(LAYERS):
                start = (2 * LAYERS + l) * NR
                here = [NC - far * U for far in (at, CHIPS - 1 - at)]
                pushed(2, l, 2 * NR + sum(min(max(n - start, 0), NR) for n in here))

    lane = seed.at[pl.ds(0, U)]
    for d in range(2):
        @pl.when((c == d) & (qs[d] < CHIPS - 1))
        def _():
            wait_local(lane, seed_sem.at[0])
            wait_local(lane, seed_sem.at[2])

        @pl.when((c != d) & (qs[d] < CHIPS - 1))
        def _():
            wait_local(lane, seed_sem.at[1])


def place(still, moved, *refs):
    n, k = still, len(moved)
    fresh = sum(old is None for _, old in moved)
    held, src = refs[:n], refs[n : n + k]
    outs = refs[n + k + (k - fresh) :]
    held_out, dst, (ring, held_sem, in_sem, out_sem) = outs[:n], outs[n : n + k], (outs[n + k : -3], *outs[-3:])
    moves = []
    for i, (pieces, _) in enumerate(moved):
        for at, buf in pieces:
            s = len(moves) % MOVE
            moves.append((pltpu.make_async_copy(src[i].at[at], ring[buf].at[s], in_sem.at[s]),
                          pltpu.make_async_copy(ring[buf].at[s], dst[i].at[at], out_sem.at[s])))
    copies = []
    for i in range(n):
        parts = 4 if held[i].dtype == jnp.bfloat16 else 1
        rows = held[i].shape[1] // parts
        for l in range(LAYERS):
            for p in range(parts):
                at = (l, pl.ds(p * rows, rows), slice(None))
                copies.append(pltpu.make_async_copy(held[i].at[at], held_out[i].at[at], held_sem.at[i]))
    ahead = MOVE // 2
    if not moves:
        for copy in copies:
            copy.start()
    for i in range(len(moves) + ahead if moves else 0):
        if i < len(moves):
            if i >= MOVE:
                moves[i - MOVE][1].wait()
            moves[i][0].start()
        if i == ahead - 1:
            for copy in copies:
                copy.start()
        if i >= ahead:
            moves[i - ahead][0].wait()
            moves[i - ahead][1].start()
    for _, out in moves[-MOVE:]:
        out.wait()
    for i in range(n):
        pltpu.make_async_copy(held[i], held_out[i], held_sem.at[i]).wait()


def fill(geo, rounds, old, *refs):
    C, CD, NR, NC, _ = geo
    R = C // CD
    n = len(rounds)
    got, swapped, new, sem = refs[:n], refs[n : 2 * n], refs[2 * n], refs[2 * n + 1]
    me = lax.axis_index("dp")
    z, c = me // 2, me % 2
    qs = (z, CHIPS - 1 - z)
    h = ROWS * R

    def each(body):
        for a, r in enumerate(rounds):
            for d in range(2):
                @pl.when(qs[d] >= r)
                def _(a=a, r=r, d=d):
                    body(a, r, d, sem.at[a * 2 + d])

    def put(a, r, d, sem):
        for lane in range(2):
            for i in range(U):
                j = NC - qs[d] * U + (r - 1) * U + i - 2 * LAYERS * NR
                block = (0 if d == 0 else CHIPS - 1) * 2 + lane
                to = new.at[j // NR, pl.ds(pl.multiple_of((block * NR + j % NR) * h, h), h), :]
                for mine, src in ((True, got[a]), (False, swapped[a])):
                    @pl.when((c == d) == mine)
                    def _(src=src, to=to, lane=lane, i=i):
                        pltpu.make_async_copy(src.at[lane * U + i], to, sem).start()

    def end(a, r, d, sem):
        pltpu.make_async_copy(got[a], got[a], sem).wait()

    each(put)
    each(end)


def step(*arrays):
    _, w, m, v = (arrays[i : i + 3] for i in (0, 3, 6, 9))
    C, CD = w[0].shape[2], w[2].shape[2]
    NR = m[0].shape[1] // ROWS
    NC = NR * LAYERS * 3
    CB = 384 if CD % 384 == 0 else CD
    geo = (C, CD, NR, NC, CB)
    E = 4 * NC
    bf, f32 = jnp.bfloat16, jnp.float32
    hbm, vmem = pl.BlockSpec(memory_space=pl.ANY), pl.BlockSpec(memory_space=pltpu.VMEM)
    outs = [pltpu.VMEM(x.shape, x.dtype) for x in w[:HELD]] + [jax.ShapeDtypeStruct(x.shape, x.dtype) for x in w[HELD:]]
    outs += [pltpu.VMEM(x.shape, x.dtype) for x in (*m, *v)]
    piece = (2 * U, ROWS * (C // CD), CD)
    outs += [pltpu.VMEM(piece, bf)]
    outs += [jax.ShapeDtypeStruct((LAYERS, CHIPS, *x.shape[1:]), bf) for x in m]
    dma = pltpu.SemaphoreType.DMA
    got = pl.pallas_call(
        functools.partial(kernel, geo),
        out_shape=outs,
        in_specs=[hbm] * 12,
        out_specs=[vmem] * HELD + [hbm] * (3 - HELD) + [vmem] * 7 + [hbm] * 3,
        scratch_shapes=[
            pltpu.VMEM((2, SLOTS, ROWS, C), bf),
            pltpu.VMEM((2, RING, ROWS, C), bf),
            pltpu.VMEM((2, RING, ROWS, C), bf),
            pltpu.VMEM((2, K, ROWS, C), bf),
            pltpu.VMEM((FR, ROWS, C), f32),
            pltpu.VMEM((FR, ROWS, C), f32),
            pltpu.VMEM((FR, ROWS, C), bf),
            pltpu.VMEM((FR, ROWS, C), bf),
            dma((2, SLOTS)),
            pltpu.SemaphoreType.REGULAR((2,)),
            dma((2, K)),
            dma((2, KA)),
            dma((2, RING)),
            dma((2, RING)),
            dma((E // PG,)),
            dma((PS,)),
            dma((2, RING)),
            dma((3, FR)),
            dma(()),
            dma((3 * LAYERS,)),
            dma((3 * LAYERS,)),
            dma((3,)),
        ],
        compiler_params=pltpu.CompilerParams(collective_id=0, has_side_effects=True, vmem_limit_bytes=VMEM_LIMIT),
        name="step",
    )(*arrays)
    seed = got[9]
    local = pltpu.CompilerParams(vmem_limit_bytes=VMEM_LIMIT)

    def onward(first):
        there = [(2 * p, 2 * p + 2) for p in range(first, CHIPS - 1)]
        return there + [(2 * CHIPS - 1 - a, 2 * CHIPS - 1 - b) for a, b in there]

    got_by, swapped = [], []
    for r in range(1, HOPS + 1):
        seed = lax.ppermute(seed, "dp", onward(r - 1))
        seed = pltpu.with_memory_space_constraint(seed, pltpu.VMEM)
        got_by.append(seed)
        other = lax.ppermute(seed, "dp", [(i, i ^ 1) for i in range(2 * CHIPS)])
        swapped.append(pltpu.with_memory_space_constraint(other, pltpu.VMEM))

    def cost(n):
        return pl.CostEstimate(flops=n, bytes_accessed=n, transcendentals=0)

    def pieces(k, first, last):
        n = w[k].shape[1] // CUTS
        return [((i // CUTS, pl.ds(i % CUTS * n, n), slice(None)), 0 if k < 2 else 1) for i in range(first, last)]

    def move(still, moved):
        types = [jax.ShapeDtypeStruct(x.shape, x.dtype) for x in still]
        types += [jax.ShapeDtypeStruct(w[k].shape, bf) for k, _, _ in moved]
        olds = [old for _, _, old in moved if old is not None]
        begin = len(still) + len(moved)
        where = [len(still) + i for i, (_, _, old) in enumerate(moved) if old is not None]
        return pl.pallas_call(
            functools.partial(place, len(still), [(p, old) for _, p, old in moved]),
            out_shape=types,
            in_specs=[vmem] * len(still) + [hbm] * (len(moved) + len(olds)),
            out_specs=[hbm] * len(types),
            scratch_shapes=[
                pltpu.VMEM((MOVE, w[0].shape[1] // CUTS, C), bf),
                pltpu.VMEM((MOVE, w[2].shape[1] // CUTS, CD), bf),
                dma((max(len(still), 1),)),
                dma((MOVE,)),
                dma((MOVE,)),
            ],
            input_output_aliases={begin + i: to for i, to in enumerate(where)},
            compiler_params=local,
            cost_estimate=cost(4 * w[0].size),
        )(*(pltpu.with_memory_space_constraint(x, pltpu.VMEM) for x in still),
          *(pltpu.with_memory_space_constraint(got[k], pltpu.HBM) for k, _, _ in moved), *olds)

    def take(rounds, old):
        n = len(rounds)
        return pl.pallas_call(
            functools.partial(fill, geo, rounds),
            out_shape=jax.ShapeDtypeStruct(old.shape, bf),
            in_specs=[hbm] + [vmem] * (2 * n),
            out_specs=hbm,
            scratch_shapes=[dma((2 * n,))],
            input_output_aliases={0: 0},
            compiler_params=local,
            cost_estimate=cost(4 * n * 6 * U * 1000),
        )(old, *(got_by[r - 1] for r in rounds), *(swapped[r - 1] for r in rounds))

    gate, *moments = move([got[0], *got[3:9]], [])
    (up,) = move([], [(1, pieces(1, 0, CUTS), None)])
    down, up = move([got[2]], [(1, pieces(1, CUTS, 2 * CUTS), up)])
    down = take(tuple(range(1, HOPS)), down)
    down = take((HOPS,), down)
    return (gate, up, down, *moments)


def solution(mesh):
    all_of, cut = P(None, None, None), P(None, "dp", None)

    return jax.shard_map(
        step,
        mesh=mesh,
        in_specs=(P(("rep", "dp"), None, None, None),) * 3 + (all_of,) * 3 + (cut,) * 6,
        out_specs=(P("rep", None, None),) * 3 + (P("rep", "dp", None),) * 6,
        check_vma=False,
    )
```

```python
import functools

import jax
import jax.numpy as jnp
from jax import lax
from jax.experimental import pallas as pl
from jax.experimental.pallas import tpu as pltpu
from jax.sharding import PartitionSpec as P


MESH = pl.DeviceIdType.MESH
ROWS = 16
LAYERS = 2
CHIPS = 4
K = 4
KA = 4
LAG = 2
END = 3
D = 2
PF = 2
RING = 3
FR = 2
CUTS = 24
SPLIT = 26
MOVE = 8
U = 4
HOPS = CHIPS - 1
VMEM_LIMIT = 10 << 20
HELD = 1
PRE = 4
PS = 8
PG = 9
G = 6
SLOTS = 18


def adamw(w, m, v, g):
    m = 0.9 * m + 0.1 * g
    v = 0.95 * v + 0.05 * g * g
    step = m * lax.rsqrt(v + 1e-8) + 0.1 * w
    return (w - 0.02 * step).astype(jnp.bfloat16), m, v


def kernel(geo, *refs):
    C, CD, NR, NC, CB = geo
    R = C // CD
    E = 4 * NC
    g, w, m, v = refs[0:3], refs[3:6], refs[6:9], refs[9:12]
    W, M, V, seed, PT = refs[12:15], refs[15:18], refs[18:21], refs[21], refs[22:25]
    (land, own, par, out, mb, vb, wb, wn, recv, credits, send, gsend, ownsem, parsem, d2d_recv, d2d_send, d2d_first, ld_sem, ww_sem,
     ag_recv, ag_send, seed_sem) = refs[25:]
    rep = lax.axis_index("rep")
    me = lax.axis_index("dp")
    z, c = me // 2, me % 2
    partner = (rep, z * 2 + 1 - c)
    nexts = ((rep, jnp.minimum(z + 1, CHIPS - 1) * 2 + c), (rep, jnp.maximum(z - 1, 0) * 2 + c))
    qs = (z, CHIPS - 1 - z)

    def split(j):
        mat = j // NR
        return mat // LAYERS, mat % LAYERS, j % NR

    def by_weight(j, body):
        k, l, r = split(j)
        for i in range(3):
            @pl.when(k == i)
            def _(i=i):
                body(i, l, r)

    def rows(i, dev, r):
        n = ROWS if i < 2 else ROWS * R
        return pl.ds(pl.multiple_of((dev * NR + r) * n, n), n)

    def load(i, src, dst, sem):
        if i < 2:
            pltpu.make_async_copy(src, dst, sem).start()
        else:
            for s in range(R):
                pltpu.make_async_copy(src.at[pl.ds(s * ROWS, ROWS), :], dst.at[:, pl.ds(s * CD, CD)], sem).start()

    def save(i, src, dst, sem):
        if i < 2:
            pltpu.make_async_copy(src, dst, sem).start()
        else:
            for s in range(R):
                pltpu.make_async_copy(src.at[:, pl.ds(s * CD, CD)], dst.at[pl.ds(s * ROWS, ROWS), :], sem).start()

    def wait_local(buf, sem):
        pltpu.make_async_copy(buf, buf, sem).wait()

    def decode(e):
        p = e - NC
        x = p - D
        first, last, head, tail = p < 0, p >= 2 * NC, p < D, p >= 2 * NC - D
        beta = jnp.where(first, 3, jnp.where(last, 0, jnp.where(head, 2, jnp.where(tail, 1, 1 + x % 2))))
        mid = jnp.where(x % 2 == 0, x // 2, D + x // 2)
        j = jnp.where(first, e, jnp.where(last, p - 2 * NC, jnp.where(head, p, jnp.where(tail, p - NC, mid))))
        return beta, j

    def sums(e, q):
        beta, j = decode(e)
        return (e >= 0) & (e < E) & ((q < beta) | ((q == beta) & (beta % 2 == 1))), beta, j

    def pair_index(b, i):
        n = NC // PG
        return jnp.where((b == 0) | (b == 3), 2 * i + jnp.where(b == 0, 1, 0), 2 * n + 2 * i + jnp.where(b == 1, 1, 0))

    def pair_group(i):
        n = NC // PG
        late = i >= 2 * n
        odd = i % 2
        b = jnp.where(late, 2 - odd, 3 - 3 * odd)
        return b, jnp.where(late, i - 2 * n, i) // 2

    def pair_wait(sem):
        many = land.at[0, pl.ds(0, PG)]
        pltpu.make_async_copy(many, many, sem).wait()

    def pair_push(i):
        @pl.when(i < 4 * NC // PG)
        def _():
            @pl.when(i >= PS)
            def _():
                pair_wait(d2d_send.at[i % PS])

            b, group = pair_group(i)

            def go(k, l, r):
                n = (ROWS if k < 2 else ROWS * R) * PG
                src = pl.ds(pl.multiple_of(((2 * b + 1 - c) * NR + r) * (n // PG), n), n)
                dst = pl.ds(pl.multiple_of(r * (n // PG), n), n)
                pltpu.make_async_remote_copy(
                    g[k].at[0, l, src, :], PT[k].at[l, b, dst, :], d2d_send.at[i % PS], d2d_recv.at[i],
                    device_id=partner, device_id_type=MESH).start()

            by_weight(group * PG, go)

    def first_push(d, e):
        b = (CHIPS - 1) * (1 - d)
        pltpu.make_async_remote_copy(
            g[0].at[0, 0, rows(0, 2 * b + 1 - c, e), :], par.at[d, e], d2d_first.at[d, e], parsem.at[d, e],
            device_id=partner, device_id_type=MESH).start()

    def prefetch(d, e):
        need, beta, j = sums(e, qs[d])
        b = beta if d == 0 else CHIPS - 1 - beta

        @pl.when(need)
        def _():
            s = e % RING
            by_weight(j, lambda k, l, r: load(k, g[k].at[0, l, rows(k, 2 * b + c, r), :], own.at[d, s], ownsem.at[d, s]))

            @pl.when((j % PG == 0) & (e >= RING) | (e == RING))
            def _():
                pair_wait(d2d_recv.at[pair_index(b, j // PG)])

            @pl.when(e >= RING)
            def _():
                by_weight(j, lambda k, l, r: load(k, PT[k].at[l, b, rows(k, 0, r), :], par.at[d, s], parsem.at[d, s]))

    def step_load(j):
        @pl.when(j < NC)
        def _():
            s = j % FR

            def go(k, l, r):
                load(k, m[k].at[l, rows(k, 0, r), :], mb.at[s], ld_sem.at[0, s])
                load(k, v[k].at[l, rows(k, 0, r), :], vb.at[s], ld_sem.at[1, s])
                load(k, w[k].at[l, rows(k, me, r), :], wb.at[s], ld_sem.at[2, s])

            by_weight(j, go)

    def wait_sum(d, n):
        pltpu.make_async_copy(out.at[d, 0], out.at[d, 0], send.at[d, n % K]).wait()

    def wait_gather(d, n):
        pltpu.make_async_copy(out.at[d, 0], out.at[d, 0], gsend.at[d, n % KA]).wait()

    def wait_recv(d, n):
        pltpu.make_async_copy(land.at[d, 0], land.at[d, 0], recv.at[d, n % SLOTS]).wait()

    def credit(d, n):
        @pl.when((n >= SLOTS) & (n % G == 0))
        def _():
            pl.semaphore_wait(credits.at[d], 1)

    def columns(body):
        def step(i, _):
            body(pl.ds(pl.multiple_of(i * CB, CB), CB))
            return 0

        lax.fori_loop(0, C // CB, step, 0)

    def weight(k, l, dev, r):
        return W[k].at[l, rows(k, dev, r), :]

    def gather_send(d, j, dev, i, n):
        @pl.when(i >= KA)
        def _():
            wait_gather(d, i)

        credit(d, n)

        def go(k, l, r):
            pltpu.make_async_remote_copy(
                weight(k, l, dev, r), weight(k, l, dev, r), gsend.at[d, i % KA], recv.at[d, n % SLOTS],
                device_id=nexts[d], device_id_type=MESH).start()

        by_weight(j, go)

    def partner_push(j, dev):
        def go(k, l, r):
            mat = k * LAYERS + l
            pltpu.make_async_remote_copy(
                weight(k, l, dev, r), weight(k, l, dev, r), ag_send.at[mat], ag_recv.at[mat],
                device_id=partner, device_id_type=MESH).start()

        by_weight(j, go)

    def handle(d, t):
        q = qs[d]
        e = t - LAG * q - jnp.where(q == CHIPS - 1, END, 0)
        sent = NC - (q + 1) * U
        came = jnp.where(q == 0, sent, sent + U)
        valid = (e >= 0) & (e < 3 * NC + came)
        beta, j = decode(e)
        b = beta if d == 0 else CHIPS - 1 - beta
        dev = 2 * b + c
        s = e % RING

        @pl.when(valid & (q < beta))
        def _():
            wait_local(own.at[d, s], ownsem.at[d, s])
            wait_local(par.at[d, s], parsem.at[d, s])
            i = jnp.where((q == 1) & (beta == 2), NC + j, e)
            o = i % K

            @pl.when(i >= K)
            def _():
                wait_sum(d, i)

            credit(d, e)

            @pl.when(q == 0)
            def _():
                def body(col):
                    total = own[d, s, :, col].astype(jnp.float32) + par[d, s, :, col].astype(jnp.float32)
                    out[d, o, :, col] = total.astype(jnp.bfloat16)

                columns(body)

            @pl.when(q > 0)
            def _():
                wait_recv(d, e)

                def body(col):
                    total = own[d, s, :, col].astype(jnp.float32) + par[d, s, :, col].astype(jnp.float32)
                    out[d, o, :, col] = (total + land[d, e % SLOTS, :, col].astype(jnp.float32)).astype(jnp.bfloat16)

                columns(body)

            pltpu.make_async_remote_copy(
                out.at[d, o], land.at[d, e % SLOTS], send.at[d, o], recv.at[d, e % SLOTS],
                device_id=nexts[d], device_id_type=MESH).start()

        @pl.when(valid & (q == beta) & (beta % 2 == 1))
        def _():
            f = j % FR
            wait_local(own.at[d, s], ownsem.at[d, s])
            wait_local(par.at[d, s], parsem.at[d, s])
            wait_local(mb.at[f], ld_sem.at[0, f])
            wait_local(vb.at[f], ld_sem.at[1, f])
            wait_local(wb.at[f], ld_sem.at[2, f])
            wait_recv(d, e)
            other = NC + jnp.where(j < D, j, 2 * j - D + 1)

            def update(extra, k, l, r):
                for p in range(1 if k < 2 else R):
                    rr = pl.ds(pl.multiple_of((r if k < 2 else r * R + p) * ROWS, ROWS), ROWS)
                    width = C if k < 2 else CD

                    def body(i, _, p=p, rr=rr, width=width):
                        col = pl.ds(pl.multiple_of(p * width + i * CB, CB), CB)
                        to = pl.ds(pl.multiple_of(i * CB, CB), CB)
                        total = own[d, s, :, col].astype(jnp.float32) + par[d, s, :, col].astype(jnp.float32)
                        total = total + land[d, e % SLOTS, :, col].astype(jnp.float32)
                        if extra:
                            total = total + land[1 - d, other % SLOTS, :, col].astype(jnp.float32)
                        grad = total.astype(jnp.bfloat16).astype(jnp.float32)
                        new, M[k][l, rr, to], V[k][l, rr, to] = adamw(
                            wb[f, :, col].astype(jnp.float32), mb[f, :, col], vb[f, :, col], grad)
                        if k < HELD:
                            W[k][l, rows(k, me, r), to] = new
                        else:
                            wn[f, :, col] = new
                        return 0

                    lax.fori_loop(0, width // CB, body, 0)

            @pl.when(beta == 1)
            def _():
                wait_recv(1 - d, other)
                by_weight(j, functools.partial(update, True))

            @pl.when(beta == 3)
            def _():
                by_weight(j, functools.partial(update, False))

            def put(k, l, r):
                if k >= HELD:
                    save(k, wn.at[f], weight(k, l, me, r), ww_sem)
                    wait_local(wn.at[f], ww_sem)

            by_weight(j, put)

            @pl.when(beta == 1)
            def _():
                gather_send(d, j, dev, j, e)
                gather_send(1 - d, j, dev, 2 * j, NC + 2 * j)

            partner_push(j, dev)
            step_load(j + FR - 1)

        @pl.when(valid & (q == beta) & (beta == 0))
        def _():
            gather_send(d, j, dev, j, e)

        @pl.when(valid & (q == CHIPS - 1) & (beta == 1))
        def _():
            wait_recv(d, NC + 2 * j)
            partner_push(j, dev + jnp.where(d == 0, 2, -2))

        @pl.when(valid & (q > beta) & (beta != 2))
        def _():
            two = beta == 1
            wait_recv(d, jnp.where(two & (q == CHIPS - 1), NC + 2 * j + 1, e))

            @pl.when((q < CHIPS - 1) & ((beta > 0) | (j < sent)))
            def _():
                i = jnp.where(q == 1, NC + j, jnp.where(two, 2 * j + 1, 2 * NC + j))
                gather_send(d, j, dev, i, jnp.where(two, NC + 2 * j + 1, e))

            partner_push(j, dev)

        i = jnp.where(q == 0, j, j - sent)

        @pl.when(valid & (beta == 0) & (q < CHIPS - 1) & (i >= 0) & (i < U))
        def _():
            _, l, r = split(sent + i)
            src, dst = weight(2, l, dev, r), seed.at[c * U + i]

            @pl.when(c == d)
            def _():
                pltpu.make_async_copy(src, dst, seed_sem.at[0]).start()

            @pl.when(c != d)
            def _():
                pltpu.make_async_remote_copy(
                    src, dst, seed_sem.at[1], seed_sem.at[2], device_id=partner, device_id_type=MESH).start()

        done = e - 2 * D

        @pl.when(valid & (q > 0) & (done >= 0) & (done % G == G - 1) & (done + 1 - G + SLOTS < 3 * NC + came))
        def _():
            pl.semaphore_signal(credits.at[d], inc=1, device_id=nexts[1 - d], device_id_type=MESH)

        prefetch(d, e + PF)

    barrier = pltpu.get_barrier_semaphore()
    pl.semaphore_signal(barrier, inc=1, device_id=partner, device_id_type=MESH)
    for d in range(2):
        @pl.when(qs[d] < CHIPS - 1)
        def _(d=d):
            pl.semaphore_signal(barrier, inc=1, device_id=nexts[d], device_id_type=MESH)
    for j in range(FR - 1):
        step_load(jnp.int32(j))
    inner = (z > 0) & (z < CHIPS - 1)
    pl.semaphore_wait(barrier, jnp.where(inner, 3, 2))

    def before(i, _):
        pair_push(i)
        return 0

    for e in range(RING):
        for d in range(2):
            first_push(d, e)
    lax.fori_loop(0, PRE, before, 0)

    def slot(i, _):
        t = i - PF
        pair_push(i + PRE)
        handle(0, t)
        handle(1, t)
        return 0

    lax.fori_loop(0, PF + E + LAG * (CHIPS - 1) + END, slot, 0)

    for d in range(2):
        @pl.when(qs[d] < CHIPS - 1)
        def _(d=d):
            for s in range(K):
                wait_sum(d, s)
            for s in range(KA):
                wait_gather(d, s)
    for s in range(PS):
        pair_wait(d2d_send.at[s])
    for e in range(RING):
        for d in range(2):
            wait_local(par.at[d, e], d2d_first.at[d, e])

    def pushed(k, l, chunks):
        if chunks:
            n = chunks * (ROWS if k < 2 else ROWS * R)
            for sem in (ag_send, ag_recv):
                pltpu.make_async_copy(W[k].at[l, pl.ds(0, n), :], W[k].at[l, pl.ds(0, n), :], sem.at[k * LAYERS + l]).wait()

    for k in range(2):
        for l in range(LAYERS):
            pushed(k, l, CHIPS * NR)
    for at in range(CHIPS):
        @pl.when(z == at)
        def _(at=at):
            for l in range(LAYERS):
                start = (2 * LAYERS + l) * NR
                here = [NC - far * U for far in (at, CHIPS - 1 - at)]
                pushed(2, l, 2 * NR + sum(min(max(n - start, 0), NR) for n in here))

    lane = seed.at[pl.ds(0, U)]
    for d in range(2):
        @pl.when((c == d) & (qs[d] < CHIPS - 1))
        def _():
            wait_local(lane, seed_sem.at[0])
            wait_local(lane, seed_sem.at[2])

        @pl.when((c != d) & (qs[d] < CHIPS - 1))
        def _():
            wait_local(lane, seed_sem.at[1])


def place(still, moved, *refs):
    n, k = still, len(moved)
    fresh = sum(old is None for _, old in moved)
    held, src = refs[:n], refs[n : n + k]
    outs = refs[n + k + (k - fresh) :]
    held_out, dst, (ring, held_sem, in_sem, out_sem) = outs[:n], outs[n : n + k], (outs[n + k : -3], *outs[-3:])
    moves = []
    for i, (pieces, _) in enumerate(moved):
        for at, buf in pieces:
            s = len(moves) % MOVE
            moves.append((pltpu.make_async_copy(src[i].at[at], ring[buf].at[s], in_sem.at[s]),
                          pltpu.make_async_copy(ring[buf].at[s], dst[i].at[at], out_sem.at[s])))
    copies = []
    for i in range(n):
        parts = 4 if held[i].dtype == jnp.bfloat16 else 1
        rows = held[i].shape[1] // parts
        for l in range(LAYERS):
            for p in range(parts):
                at = (l, pl.ds(p * rows, rows), slice(None))
                copies.append(pltpu.make_async_copy(held[i].at[at], held_out[i].at[at], held_sem.at[i]))
    ahead = MOVE // 2
    if not moves:
        for copy in copies:
            copy.start()
    for i in range(len(moves) + ahead if moves else 0):
        if i < len(moves):
            if i >= MOVE:
                moves[i - MOVE][1].wait()
            moves[i][0].start()
        if i == ahead - 1:
            for copy in copies:
                copy.start()
        if i >= ahead:
            moves[i - ahead][0].wait()
            moves[i - ahead][1].start()
    for _, out in moves[-MOVE:]:
        out.wait()
    for i in range(n):
        pltpu.make_async_copy(held[i], held_out[i], held_sem.at[i]).wait()


def fill(geo, rounds, old, *refs):
    C, CD, NR, NC, _ = geo
    R = C // CD
    n = len(rounds)
    got, swapped, new, sem = refs[:n], refs[n : 2 * n], refs[2 * n], refs[2 * n + 1]
    me = lax.axis_index("dp")
    z, c = me // 2, me % 2
    qs = (z, CHIPS - 1 - z)
    h = ROWS * R

    def each(body):
        for a, r in enumerate(rounds):
            for d in range(2):
                @pl.when(qs[d] >= r)
                def _(a=a, r=r, d=d):
                    body(a, r, d, sem.at[a * 2 + d])

    def put(a, r, d, sem):
        for lane in range(2):
            for i in range(U):
                j = NC - qs[d] * U + (r - 1) * U + i - 2 * LAYERS * NR
                block = (0 if d == 0 else CHIPS - 1) * 2 + lane
                to = new.at[j // NR, pl.ds(pl.multiple_of((block * NR + j % NR) * h, h), h), :]
                for mine, src in ((True, got[a]), (False, swapped[a])):
                    @pl.when((c == d) == mine)
                    def _(src=src, to=to, lane=lane, i=i):
                        pltpu.make_async_copy(src.at[lane * U + i], to, sem).start()

    def end(a, r, d, sem):
        pltpu.make_async_copy(got[a], got[a], sem).wait()

    each(put)
    each(end)


def step(*arrays):
    _, w, m, v = (arrays[i : i + 3] for i in (0, 3, 6, 9))
    C, CD = w[0].shape[2], w[2].shape[2]
    NR = m[0].shape[1] // ROWS
    NC = NR * LAYERS * 3
    CB = 384 if CD % 384 == 0 else CD
    geo = (C, CD, NR, NC, CB)
    E = 4 * NC
    bf, f32 = jnp.bfloat16, jnp.float32
    hbm, vmem = pl.BlockSpec(memory_space=pl.ANY), pl.BlockSpec(memory_space=pltpu.VMEM)
    outs = [pltpu.VMEM(x.shape, x.dtype) for x in w[:HELD]] + [jax.ShapeDtypeStruct(x.shape, x.dtype) for x in w[HELD:]]
    outs += [pltpu.VMEM(x.shape, x.dtype) for x in (*m, *v)]
    piece = (2 * U, ROWS * (C // CD), CD)
    outs += [pltpu.VMEM(piece, bf)]
    outs += [jax.ShapeDtypeStruct((LAYERS, CHIPS, *x.shape[1:]), bf) for x in m]
    dma = pltpu.SemaphoreType.DMA
    got = pl.pallas_call(
        functools.partial(kernel, geo),
        out_shape=outs,
        in_specs=[hbm] * 12,
        out_specs=[vmem] * HELD + [hbm] * (3 - HELD) + [vmem] * 7 + [hbm] * 3,
        scratch_shapes=[
            pltpu.VMEM((2, SLOTS, ROWS, C), bf),
            pltpu.VMEM((2, RING, ROWS, C), bf),
            pltpu.VMEM((2, RING, ROWS, C), bf),
            pltpu.VMEM((2, K, ROWS, C), bf),
            pltpu.VMEM((FR, ROWS, C), f32),
            pltpu.VMEM((FR, ROWS, C), f32),
            pltpu.VMEM((FR, ROWS, C), bf),
            pltpu.VMEM((FR, ROWS, C), bf),
            dma((2, SLOTS)),
            pltpu.SemaphoreType.REGULAR((2,)),
            dma((2, K)),
            dma((2, KA)),
            dma((2, RING)),
            dma((2, RING)),
            dma((E // PG,)),
            dma((PS,)),
            dma((2, RING)),
            dma((3, FR)),
            dma(()),
            dma((3 * LAYERS,)),
            dma((3 * LAYERS,)),
            dma((3,)),
        ],
        compiler_params=pltpu.CompilerParams(collective_id=0, has_side_effects=True, vmem_limit_bytes=VMEM_LIMIT),
        name="step",
    )(*arrays)
    seed = got[9]
    local = pltpu.CompilerParams(vmem_limit_bytes=VMEM_LIMIT)

    def onward(first):
        there = [(2 * p, 2 * p + 2) for p in range(first, CHIPS - 1)]
        return there + [(2 * CHIPS - 1 - a, 2 * CHIPS - 1 - b) for a, b in there]

    got_by, swapped = [], []
    for r in range(1, HOPS + 1):
        seed = lax.ppermute(seed, "dp", onward(r - 1))
        seed = pltpu.with_memory_space_constraint(seed, pltpu.VMEM)
        got_by.append(seed)
        other = lax.ppermute(seed, "dp", [(i, i ^ 1) for i in range(2 * CHIPS)])
        swapped.append(pltpu.with_memory_space_constraint(other, pltpu.VMEM))

    def cost(n):
        return pl.CostEstimate(flops=n, bytes_accessed=n, transcendentals=0)

    def pieces(k, first, last):
        n = w[k].shape[1] // CUTS
        return [((i // CUTS, pl.ds(i % CUTS * n, n), slice(None)), 0 if k < 2 else 1) for i in range(first, last)]

    def move(still, moved):
        types = [jax.ShapeDtypeStruct(x.shape, x.dtype) for x in still]
        types += [jax.ShapeDtypeStruct(w[k].shape, bf) for k, _, _ in moved]
        olds = [old for _, _, old in moved if old is not None]
        begin = len(still) + len(moved)
        where = [len(still) + i for i, (_, _, old) in enumerate(moved) if old is not None]
        return pl.pallas_call(
            functools.partial(place, len(still), [(p, old) for _, p, old in moved]),
            out_shape=types,
            in_specs=[vmem] * len(still) + [hbm] * (len(moved) + len(olds)),
            out_specs=[hbm] * len(types),
            scratch_shapes=[
                pltpu.VMEM((MOVE, w[0].shape[1] // CUTS, C), bf),
                pltpu.VMEM((MOVE, w[2].shape[1] // CUTS, CD), bf),
                dma((max(len(still), 1),)),
                dma((MOVE,)),
                dma((MOVE,)),
            ],
            input_output_aliases={begin + i: to for i, to in enumerate(where)},
            compiler_params=local,
            cost_estimate=cost(4 * w[0].size),
        )(*(pltpu.with_memory_space_constraint(x, pltpu.VMEM) for x in still),
          *(pltpu.with_memory_space_constraint(got[k], pltpu.HBM) for k, _, _ in moved), *olds)

    def take(rounds, old):
        n = len(rounds)
        return pl.pallas_call(
            functools.partial(fill, geo, rounds),
            out_shape=jax.ShapeDtypeStruct(old.shape, bf),
            in_specs=[hbm] + [vmem] * (2 * n),
            out_specs=hbm,
            scratch_shapes=[dma((2 * n,))],
            input_output_aliases={0: 0},
            compiler_params=local,
            cost_estimate=cost(4 * n * 6 * U * 1000),
        )(old, *(got_by[r - 1] for r in rounds), *(swapped[r - 1] for r in rounds))

    gate, *moments = move([got[0], *got[3:8]], [])
    last, up = move(got[8:9], [(1, pieces(1, 0, SPLIT), None)])
    down, up = move([got[2]], [(1, pieces(1, SPLIT, 2 * CUTS), up)])
    down = take(tuple(range(1, HOPS)), down)
    down = take((HOPS,), down)
    return (gate, up, down, *moments, last)


def solution(mesh):
    all_of, cut = P(None, None, None), P(None, "dp", None)

    return jax.shard_map(
        step,
        mesh=mesh,
        in_specs=(P(("rep", "dp"), None, None, None),) * 3 + (all_of,) * 3 + (cut,) * 6,
        out_specs=(P("rep", None, None),) * 3 + (P("rep", "dp", None),) * 6,
        check_vma=False,
    )
```

```python
import functools

import jax
import jax.numpy as jnp
from jax import lax
from jax.experimental import pallas as pl
from jax.experimental.pallas import tpu as pltpu
from jax.sharding import PartitionSpec as P


MESH = pl.DeviceIdType.MESH
ROWS = 16
LAYERS = 2
CHIPS = 4
K = 4
KA = 4
LAG = 2
END = 3
D = 2
PF = 2
RING = 3
FR = 2
CUTS = 12
SPLIT = 13
MOVE = 10
U = (4, 3)
HOPS = CHIPS - 1
VMEM_LIMIT = 10 << 20
HELD = 1
PRE = 4
PS = 8
PG = 9
G = 6
SLOTS = 18


def adamw(w, m, v, g):
    m = 0.9 * m + 0.1 * g
    v = 0.95 * v + 0.05 * g * g
    step = m * lax.rsqrt(v + 1e-8) + 0.1 * w
    return (w - 0.02 * step).astype(jnp.bfloat16), m, v


def kernel(geo, *refs):
    C, CD, NR, NC, CB = geo
    R = C // CD
    E = 4 * NC
    g, w, m, v = refs[0:3], refs[3:6], refs[6:9], refs[9:12]
    W, M, V, seed, PT = refs[12:15], refs[15:18], refs[18:21], refs[21], refs[22:25]
    (land, own, par, out, mb, vb, wb, wn, recv, credits, send, gsend, ownsem, parsem, d2d_recv, d2d_send, d2d_first, ld_sem, ww_sem,
     ag_recv, ag_send, seed_sem) = refs[25:]
    rep = lax.axis_index("rep")
    me = lax.axis_index("dp")
    z, c = me // 2, me % 2
    partner = (rep, z * 2 + 1 - c)
    nexts = ((rep, jnp.minimum(z + 1, CHIPS - 1) * 2 + c), (rep, jnp.maximum(z - 1, 0) * 2 + c))
    qs = (z, CHIPS - 1 - z)

    def split(j):
        mat = j // NR
        return mat // LAYERS, mat % LAYERS, j % NR

    def by_weight(j, body):
        k, l, r = split(j)
        for i in range(3):
            @pl.when(k == i)
            def _(i=i):
                body(i, l, r)

    def rows(i, dev, r):
        n = ROWS if i < 2 else ROWS * R
        return pl.ds(pl.multiple_of((dev * NR + r) * n, n), n)

    def load(i, src, dst, sem):
        if i < 2:
            pltpu.make_async_copy(src, dst, sem).start()
        else:
            for s in range(R):
                pltpu.make_async_copy(src.at[pl.ds(s * ROWS, ROWS), :], dst.at[:, pl.ds(s * CD, CD)], sem).start()

    def save(i, src, dst, sem):
        if i < 2:
            pltpu.make_async_copy(src, dst, sem).start()
        else:
            for s in range(R):
                pltpu.make_async_copy(src.at[:, pl.ds(s * CD, CD)], dst.at[pl.ds(s * ROWS, ROWS), :], sem).start()

    def wait_local(buf, sem):
        pltpu.make_async_copy(buf, buf, sem).wait()

    def decode(e):
        p = e - NC
        x = p - D
        first, last, head, tail = p < 0, p >= 2 * NC, p < D, p >= 2 * NC - D
        beta = jnp.where(first, 3, jnp.where(last, 0, jnp.where(head, 2, jnp.where(tail, 1, 1 + x % 2))))
        mid = jnp.where(x % 2 == 0, x // 2, D + x // 2)
        j = jnp.where(first, e, jnp.where(last, p - 2 * NC, jnp.where(head, p, jnp.where(tail, p - NC, mid))))
        return beta, j

    def sums(e, q):
        beta, j = decode(e)
        return (e >= 0) & (e < E) & ((q < beta) | ((q == beta) & (beta % 2 == 1))), beta, j

    def pair_index(b, i):
        n = NC // PG
        return jnp.where((b == 0) | (b == 3), 2 * i + jnp.where(b == 0, 1, 0), 2 * n + 2 * i + jnp.where(b == 1, 1, 0))

    def pair_group(i):
        n = NC // PG
        late = i >= 2 * n
        odd = i % 2
        b = jnp.where(late, 2 - odd, 3 - 3 * odd)
        return b, jnp.where(late, i - 2 * n, i) // 2

    def pair_wait(sem):
        many = land.at[0, pl.ds(0, PG)]
        pltpu.make_async_copy(many, many, sem).wait()

    def pair_push(i):
        @pl.when(i < 4 * NC // PG)
        def _():
            @pl.when(i >= PS)
            def _():
                pair_wait(d2d_send.at[i % PS])

            b, group = pair_group(i)

            def go(k, l, r):
                n = (ROWS if k < 2 else ROWS * R) * PG
                src = pl.ds(pl.multiple_of(((2 * b + 1 - c) * NR + r) * (n // PG), n), n)
                dst = pl.ds(pl.multiple_of(r * (n // PG), n), n)
                pltpu.make_async_remote_copy(
                    g[k].at[0, l, src, :], PT[k].at[l, b, dst, :], d2d_send.at[i % PS], d2d_recv.at[i],
                    device_id=partner, device_id_type=MESH).start()

            by_weight(group * PG, go)

    def first_push(d, e):
        b = (CHIPS - 1) * (1 - d)
        pltpu.make_async_remote_copy(
            g[0].at[0, 0, rows(0, 2 * b + 1 - c, e), :], par.at[d, e], d2d_first.at[d, e], parsem.at[d, e],
            device_id=partner, device_id_type=MESH).start()

    def prefetch(d, e):
        need, beta, j = sums(e, qs[d])
        b = beta if d == 0 else CHIPS - 1 - beta

        @pl.when(need)
        def _():
            s = e % RING
            by_weight(j, lambda k, l, r: load(k, g[k].at[0, l, rows(k, 2 * b + c, r), :], own.at[d, s], ownsem.at[d, s]))

            @pl.when((j % PG == 0) & (e >= RING) | (e == RING))
            def _():
                pair_wait(d2d_recv.at[pair_index(b, j // PG)])

            @pl.when(e >= RING)
            def _():
                by_weight(j, lambda k, l, r: load(k, PT[k].at[l, b, rows(k, 0, r), :], par.at[d, s], parsem.at[d, s]))

    def step_load(j):
        @pl.when(j < NC)
        def _():
            s = j % FR

            def go(k, l, r):
                load(k, m[k].at[l, rows(k, 0, r), :], mb.at[s], ld_sem.at[0, s])
                load(k, v[k].at[l, rows(k, 0, r), :], vb.at[s], ld_sem.at[1, s])
                load(k, w[k].at[l, rows(k, me, r), :], wb.at[s], ld_sem.at[2, s])

            by_weight(j, go)

    def wait_sum(d, n):
        pltpu.make_async_copy(out.at[d, 0], out.at[d, 0], send.at[d, n % K]).wait()

    def wait_gather(d, n):
        pltpu.make_async_copy(out.at[d, 0], out.at[d, 0], gsend.at[d, n % KA]).wait()

    def wait_recv(d, n):
        pltpu.make_async_copy(land.at[d, 0], land.at[d, 0], recv.at[d, n % SLOTS]).wait()

    def credit(d, n):
        @pl.when((n >= SLOTS) & (n % G == 0))
        def _():
            pl.semaphore_wait(credits.at[d], 1)

    def columns(body):
        def step(i, _):
            body(pl.ds(pl.multiple_of(i * CB, CB), CB))
            return 0

        lax.fori_loop(0, C // CB, step, 0)

    def weight(k, l, dev, r):
        return W[k].at[l, rows(k, dev, r), :]

    def gather_send(d, j, dev, i, n):
        @pl.when(i >= KA)
        def _():
            wait_gather(d, i)

        credit(d, n)

        def go(k, l, r):
            pltpu.make_async_remote_copy(
                weight(k, l, dev, r), weight(k, l, dev, r), gsend.at[d, i % KA], recv.at[d, n % SLOTS],
                device_id=nexts[d], device_id_type=MESH).start()

        by_weight(j, go)

    def partner_push(j, dev):
        def go(k, l, r):
            mat = k * LAYERS + l
            pltpu.make_async_remote_copy(
                weight(k, l, dev, r), weight(k, l, dev, r), ag_send.at[mat], ag_recv.at[mat],
                device_id=partner, device_id_type=MESH).start()

        by_weight(j, go)

    def handle(d, t):
        q = qs[d]
        e = t - LAG * q - jnp.where(q == CHIPS - 1, END, 0)
        count = jnp.where(c == 0, U[0], U[1])
        sent = NC - (q + 1) * count
        came = jnp.where(q == 0, sent, sent + count)
        valid = (e >= 0) & (e < 3 * NC + came)
        beta, j = decode(e)
        b = beta if d == 0 else CHIPS - 1 - beta
        dev = 2 * b + c
        s = e % RING

        @pl.when(valid & (q < beta))
        def _():
            wait_local(own.at[d, s], ownsem.at[d, s])
            wait_local(par.at[d, s], parsem.at[d, s])
            i = jnp.where((q == 1) & (beta == 2), NC + j, e)
            o = i % K

            @pl.when(i >= K)
            def _():
                wait_sum(d, i)

            credit(d, e)

            @pl.when(q == 0)
            def _():
                def body(col):
                    total = own[d, s, :, col].astype(jnp.float32) + par[d, s, :, col].astype(jnp.float32)
                    out[d, o, :, col] = total.astype(jnp.bfloat16)

                columns(body)

            @pl.when(q > 0)
            def _():
                wait_recv(d, e)

                def body(col):
                    total = own[d, s, :, col].astype(jnp.float32) + par[d, s, :, col].astype(jnp.float32)
                    out[d, o, :, col] = (total + land[d, e % SLOTS, :, col].astype(jnp.float32)).astype(jnp.bfloat16)

                columns(body)

            pltpu.make_async_remote_copy(
                out.at[d, o], land.at[d, e % SLOTS], send.at[d, o], recv.at[d, e % SLOTS],
                device_id=nexts[d], device_id_type=MESH).start()

        @pl.when(valid & (q == beta) & (beta % 2 == 1))
        def _():
            f = j % FR
            wait_local(own.at[d, s], ownsem.at[d, s])
            wait_local(par.at[d, s], parsem.at[d, s])
            wait_local(mb.at[f], ld_sem.at[0, f])
            wait_local(vb.at[f], ld_sem.at[1, f])
            wait_local(wb.at[f], ld_sem.at[2, f])
            wait_recv(d, e)
            other = NC + jnp.where(j < D, j, 2 * j - D + 1)

            def update(extra, k, l, r):
                for p in range(1 if k < 2 else R):
                    rr = pl.ds(pl.multiple_of((r if k < 2 else r * R + p) * ROWS, ROWS), ROWS)
                    width = C if k < 2 else CD

                    def body(i, _, p=p, rr=rr, width=width):
                        col = pl.ds(pl.multiple_of(p * width + i * CB, CB), CB)
                        to = pl.ds(pl.multiple_of(i * CB, CB), CB)
                        total = own[d, s, :, col].astype(jnp.float32) + par[d, s, :, col].astype(jnp.float32)
                        total = total + land[d, e % SLOTS, :, col].astype(jnp.float32)
                        if extra:
                            total = total + land[1 - d, other % SLOTS, :, col].astype(jnp.float32)
                        grad = total.astype(jnp.bfloat16).astype(jnp.float32)
                        new, M[k][l, rr, to], V[k][l, rr, to] = adamw(
                            wb[f, :, col].astype(jnp.float32), mb[f, :, col], vb[f, :, col], grad)
                        if k < HELD:
                            W[k][l, rows(k, me, r), to] = new
                        else:
                            wn[f, :, col] = new
                        return 0

                    lax.fori_loop(0, width // CB, body, 0)

            @pl.when(beta == 1)
            def _():
                wait_recv(1 - d, other)
                by_weight(j, functools.partial(update, True))

            @pl.when(beta == 3)
            def _():
                by_weight(j, functools.partial(update, False))

            def put(k, l, r):
                if k >= HELD:
                    save(k, wn.at[f], weight(k, l, me, r), ww_sem)
                    wait_local(wn.at[f], ww_sem)

            by_weight(j, put)

            @pl.when(beta == 1)
            def _():
                gather_send(d, j, dev, j, e)
                gather_send(1 - d, j, dev, 2 * j, NC + 2 * j)

            partner_push(j, dev)
            step_load(j + FR - 1)

        @pl.when(valid & (q == beta) & (beta == 0))
        def _():
            gather_send(d, j, dev, j, e)

        @pl.when(valid & (q == CHIPS - 1) & (beta == 1))
        def _():
            wait_recv(d, NC + 2 * j)
            partner_push(j, dev + jnp.where(d == 0, 2, -2))

        @pl.when(valid & (q > beta) & (beta != 2))
        def _():
            two = beta == 1
            wait_recv(d, jnp.where(two & (q == CHIPS - 1), NC + 2 * j + 1, e))

            @pl.when((q < CHIPS - 1) & ((beta > 0) | (j < sent)))
            def _():
                i = jnp.where(q == 1, NC + j, jnp.where(two, 2 * j + 1, 2 * NC + j))
                gather_send(d, j, dev, i, jnp.where(two, NC + 2 * j + 1, e))

            partner_push(j, dev)

        i = jnp.where(q == 0, j, j - sent)

        @pl.when(valid & (beta == 0) & (q < CHIPS - 1) & (i >= 0) & (i < count))
        def _():
            _, l, r = split(sent + i)
            src, dst = weight(2, l, dev, r), seed.at[c * U[0] + i]

            @pl.when(c == d)
            def _():
                pltpu.make_async_copy(src, dst, seed_sem.at[0]).start()

            @pl.when(c != d)
            def _():
                pltpu.make_async_remote_copy(
                    src, dst, seed_sem.at[1], seed_sem.at[2], device_id=partner, device_id_type=MESH).start()

        done = e - 2 * D

        @pl.when(valid & (q > 0) & (done >= 0) & (done % G == G - 1) & (done + 1 - G + SLOTS < 3 * NC + came))
        def _():
            pl.semaphore_signal(credits.at[d], inc=1, device_id=nexts[1 - d], device_id_type=MESH)

        prefetch(d, e + PF)

    barrier = pltpu.get_barrier_semaphore()
    pl.semaphore_signal(barrier, inc=1, device_id=partner, device_id_type=MESH)
    for d in range(2):
        @pl.when(qs[d] < CHIPS - 1)
        def _(d=d):
            pl.semaphore_signal(barrier, inc=1, device_id=nexts[d], device_id_type=MESH)
    for j in range(FR - 1):
        step_load(jnp.int32(j))
    inner = (z > 0) & (z < CHIPS - 1)
    pl.semaphore_wait(barrier, jnp.where(inner, 3, 2))

    def before(i, _):
        pair_push(i)
        return 0

    for e in range(RING):
        for d in range(2):
            first_push(d, e)
    lax.fori_loop(0, PRE, before, 0)

    def slot(i, _):
        t = i - PF
        pair_push(i + PRE)
        handle(0, t)
        handle(1, t)
        return 0

    lax.fori_loop(0, PF + E + LAG * (CHIPS - 1) + END, slot, 0)

    for d in range(2):
        @pl.when(qs[d] < CHIPS - 1)
        def _(d=d):
            for s in range(K):
                wait_sum(d, s)
            for s in range(KA):
                wait_gather(d, s)
    for s in range(PS):
        pair_wait(d2d_send.at[s])
    for e in range(RING):
        for d in range(2):
            wait_local(par.at[d, e], d2d_first.at[d, e])

    def pushed(k, l, sem, chunks):
        if chunks:
            n = chunks * (ROWS if k < 2 else ROWS * R)
            some = W[k].at[l, pl.ds(0, n), :]
            pltpu.make_async_copy(some, some, sem.at[k * LAYERS + l]).wait()

    for k in range(2):
        for l in range(LAYERS):
            for sem in (ag_send, ag_recv):
                pushed(k, l, sem, CHIPS * NR)
    for at in range(CHIPS):
        for mine in range(2):
            @pl.when((z == at) & (c == mine))
            def _(at=at, mine=mine):
                for sem, lane in ((ag_send, mine), (ag_recv, 1 - mine)):
                    here = [NC - far * U[lane] for far in (at, CHIPS - 1 - at)]
                    for l in range(LAYERS):
                        start = (2 * LAYERS + l) * NR
                        pushed(2, l, sem, 2 * NR + sum(min(max(n - start, 0), NR) for n in here))

    for d in range(2):
        own_lane, other_lane = seed.at[pl.ds(0, U[d])], seed.at[pl.ds(0, U[1 - d])]

        @pl.when((c == d) & (qs[d] < CHIPS - 1))
        def _(own_lane=own_lane, other_lane=other_lane):
            wait_local(own_lane, seed_sem.at[0])
            wait_local(other_lane, seed_sem.at[2])

        @pl.when((c != d) & (qs[d] < CHIPS - 1))
        def _(other_lane=other_lane):
            wait_local(other_lane, seed_sem.at[1])


def place(still, moved, *refs):
    n, k = still, len(moved)
    fresh = sum(old is None for _, old in moved)
    held, src = refs[:n], refs[n : n + k]
    outs = refs[n + k + (k - fresh) :]
    held_out, dst, (ring, held_sem, in_sem, out_sem) = outs[:n], outs[n : n + k], (outs[n + k : -3], *outs[-3:])
    moves = []
    for i, (pieces, _) in enumerate(moved):
        for at, buf in pieces:
            s = len(moves) % MOVE
            moves.append((pltpu.make_async_copy(src[i].at[at], ring[buf].at[s], in_sem.at[s]),
                          pltpu.make_async_copy(ring[buf].at[s], dst[i].at[at], out_sem.at[s])))
    copies = []
    for i in range(n):
        parts = 4 if held[i].dtype == jnp.bfloat16 else 1
        rows = held[i].shape[1] // parts
        for l in range(LAYERS):
            for p in range(parts):
                at = (l, pl.ds(p * rows, rows), slice(None))
                copies.append(pltpu.make_async_copy(held[i].at[at], held_out[i].at[at], held_sem.at[i]))
    ahead = MOVE // 2
    if not moves:
        for copy in copies:
            copy.start()
    for i in range(len(moves) + ahead if moves else 0):
        if i < len(moves):
            if i >= MOVE:
                moves[i - MOVE][1].wait()
            moves[i][0].start()
        if i == ahead - 1:
            for copy in copies:
                copy.start()
        if i >= ahead:
            moves[i - ahead][0].wait()
            moves[i - ahead][1].start()
    for _, out in moves[-MOVE:]:
        out.wait()
    for i in range(n):
        pltpu.make_async_copy(held[i], held_out[i], held_sem.at[i]).wait()


def fill(geo, rounds, old, *refs):
    C, CD, NR, NC, _ = geo
    R = C // CD
    n = len(rounds)
    got, swapped, new, sem = refs[:n], refs[n : 2 * n], refs[2 * n], refs[2 * n + 1]
    me = lax.axis_index("dp")
    z, c = me // 2, me % 2
    qs = (z, CHIPS - 1 - z)
    h = ROWS * R

    def each(body):
        for a, r in enumerate(rounds):
            for d in range(2):
                @pl.when(qs[d] >= r)
                def _(a=a, r=r, d=d):
                    body(a, r, d, sem.at[a * 2 + d])

    def put(a, r, d, sem):
        for lane in range(2):
            for i in range(U[lane]):
                j = NC - qs[d] * U[lane] + (r - 1) * U[lane] + i - 2 * LAYERS * NR
                block = (0 if d == 0 else CHIPS - 1) * 2 + lane
                to = new.at[j // NR, pl.ds(pl.multiple_of((block * NR + j % NR) * h, h), h), :]
                for mine, src in ((True, got[a]), (False, swapped[a])):
                    @pl.when((c == d) == mine)
                    def _(src=src, to=to, lane=lane, i=i):
                        pltpu.make_async_copy(src.at[lane * U[0] + i], to, sem).start()

    def end(a, r, d, sem):
        pltpu.make_async_copy(got[a], got[a], sem).wait()

    each(put)
    each(end)


def step(*arrays):
    _, w, m, v = (arrays[i : i + 3] for i in (0, 3, 6, 9))
    C, CD = w[0].shape[2], w[2].shape[2]
    NR = m[0].shape[1] // ROWS
    NC = NR * LAYERS * 3
    CB = 384 if CD % 384 == 0 else CD
    geo = (C, CD, NR, NC, CB)
    E = 4 * NC
    bf, f32 = jnp.bfloat16, jnp.float32
    hbm, vmem = pl.BlockSpec(memory_space=pl.ANY), pl.BlockSpec(memory_space=pltpu.VMEM)
    outs = [pltpu.VMEM(x.shape, x.dtype) for x in w[:HELD]] + [jax.ShapeDtypeStruct(x.shape, x.dtype) for x in w[HELD:]]
    outs += [pltpu.VMEM(x.shape, x.dtype) for x in (*m, *v)]
    piece = (sum(U), ROWS * (C // CD), CD)
    outs += [pltpu.VMEM(piece, bf)]
    outs += [jax.ShapeDtypeStruct((LAYERS, CHIPS, *x.shape[1:]), bf) for x in m]
    dma = pltpu.SemaphoreType.DMA
    got = pl.pallas_call(
        functools.partial(kernel, geo),
        out_shape=outs,
        in_specs=[hbm] * 12,
        out_specs=[vmem] * HELD + [hbm] * (3 - HELD) + [vmem] * 7 + [hbm] * 3,
        scratch_shapes=[
            pltpu.VMEM((2, SLOTS, ROWS, C), bf),
            pltpu.VMEM((2, RING, ROWS, C), bf),
            pltpu.VMEM((2, RING, ROWS, C), bf),
            pltpu.VMEM((2, K, ROWS, C), bf),
            pltpu.VMEM((FR, ROWS, C), f32),
            pltpu.VMEM((FR, ROWS, C), f32),
            pltpu.VMEM((FR, ROWS, C), bf),
            pltpu.VMEM((FR, ROWS, C), bf),
            dma((2, SLOTS)),
            pltpu.SemaphoreType.REGULAR((2,)),
            dma((2, K)),
            dma((2, KA)),
            dma((2, RING)),
            dma((2, RING)),
            dma((E // PG,)),
            dma((PS,)),
            dma((2, RING)),
            dma((3, FR)),
            dma(()),
            dma((3 * LAYERS,)),
            dma((3 * LAYERS,)),
            dma((3,)),
        ],
        compiler_params=pltpu.CompilerParams(collective_id=0, has_side_effects=True, vmem_limit_bytes=VMEM_LIMIT),
        name="step",
    )(*arrays)
    seed = got[9]
    local = pltpu.CompilerParams(vmem_limit_bytes=VMEM_LIMIT)

    def onward(first):
        there = [(2 * p, 2 * p + 2) for p in range(first, CHIPS - 1)]
        return there + [(2 * CHIPS - 1 - a, 2 * CHIPS - 1 - b) for a, b in there]

    got_by, swapped = [], []
    for r in range(1, HOPS + 1):
        seed = lax.ppermute(seed, "dp", onward(r - 1))
        seed = pltpu.with_memory_space_constraint(seed, pltpu.VMEM)
        got_by.append(seed)
        other = lax.ppermute(seed, "dp", [(i, i ^ 1) for i in range(2 * CHIPS)])
        swapped.append(pltpu.with_memory_space_constraint(other, pltpu.VMEM))

    def cost(n):
        return pl.CostEstimate(flops=n, bytes_accessed=n, transcendentals=0)

    def pieces(k, first, last):
        n = w[k].shape[1] // CUTS
        return [((i // CUTS, pl.ds(i % CUTS * n, n), slice(None)), 0 if k < 2 else 1) for i in range(first, last)]

    def move(still, moved):
        types = [jax.ShapeDtypeStruct(x.shape, x.dtype) for x in still]
        types += [jax.ShapeDtypeStruct(w[k].shape, bf) for k, _, _ in moved]
        olds = [old for _, _, old in moved if old is not None]
        begin = len(still) + len(moved)
        where = [len(still) + i for i, (_, _, old) in enumerate(moved) if old is not None]
        return pl.pallas_call(
            functools.partial(place, len(still), [(p, old) for _, p, old in moved]),
            out_shape=types,
            in_specs=[vmem] * len(still) + [hbm] * (len(moved) + len(olds)),
            out_specs=[hbm] * len(types),
            scratch_shapes=[
                pltpu.VMEM((MOVE, w[0].shape[1] // CUTS, C), bf),
                dma((max(len(still), 1),)),
                dma((MOVE,)),
                dma((MOVE,)),
            ],
            input_output_aliases={begin + i: to for i, to in enumerate(where)},
            compiler_params=local,
            cost_estimate=cost(4 * w[0].size),
        )(*(pltpu.with_memory_space_constraint(x, pltpu.VMEM) for x in still),
          *(pltpu.with_memory_space_constraint(got[k], pltpu.HBM) for k, _, _ in moved), *olds)

    def take(rounds, old):
        n = len(rounds)
        return pl.pallas_call(
            functools.partial(fill, geo, rounds),
            out_shape=jax.ShapeDtypeStruct(old.shape, bf),
            in_specs=[hbm] + [vmem] * (2 * n),
            out_specs=hbm,
            scratch_shapes=[dma((2 * n,))],
            input_output_aliases={0: 0},
            compiler_params=local,
            cost_estimate=cost(12 * n * sum(U) * 1000),
        )(old, *(got_by[r - 1] for r in rounds), *(swapped[r - 1] for r in rounds))

    gate, *moments = move([got[0], *got[3:8]], [])
    last, up = move(got[8:9], [(1, pieces(1, 0, SPLIT), None)])
    down, up = move([got[2]], [(1, pieces(1, SPLIT, 2 * CUTS), up)])
    down = take(tuple(range(1, HOPS)), down)
    down = take((HOPS,), down)
    return (gate, up, down, *moments, last)


def solution(mesh):
    all_of, cut = P(None, None, None), P(None, "dp", None)

    return jax.shard_map(
        step,
        mesh=mesh,
        in_specs=(P(("rep", "dp"), None, None, None),) * 3 + (all_of,) * 3 + (cut,) * 6,
        out_specs=(P("rep", None, None),) * 3 + (P("rep", "dp", None),) * 6,
        check_vma=False,
    )
```
